8 devices in a mesh: dp: 1 (over z), sp: 2 (over y), beam: 4 (over x, core).
Axes of the slice: x: 2, y: 2, z: 1, core: 2. Of those that a mesh axis runs over, the one named last changes fastest.
Arguments:
- tok_emb: bfloat16 [32, 4096], P(('dp', 'beam'))
- parent: int32 [1, 32], P('dp')
- position: int32 [1], replicated
- beam_score: float32 [32], P(('dp', 'beam'))
- k_cache: bfloat16 [2, 32, 512, 8, 128], P(None, ('dp', 'beam'), 'sp')
- v_cache: bfloat16 [2, 32, 512, 8, 128], P(None, ('dp', 'beam'), 'sp')
- w_query: bfloat16 [2, 4096, 4096], replicated
- w_key: bfloat16 [2, 4096, 1024], replicated
- w_value: bfloat16 [2, 4096, 1024], replicated
- w_out: bfloat16 [2, 4096, 4096], replicated
- w_gate: bfloat16 [2, 4096, 14336], replicated
- w_up: bfloat16 [2, 4096, 14336], replicated
- w_down: bfloat16 [2, 14336, 4096], replicated
- g_attn: bfloat16 [2, 4096], replicated
- g_mlp: bfloat16 [2, 4096], replicated
- g_final: bfloat16 [4096], replicated
- w_vocab: bfloat16 [4096, 32768], replicated
Outputs:
- output 1: bfloat16 [2, 32, 512, 8, 128], P(None, ('dp', 'beam'), 'sp')
- output 2: bfloat16 [2, 32, 512, 8, 128], P(None, ('dp', 'beam'), 'sp')
- output 3: float32 [32, 32768], P(('dp', 'beam'))
All inputs are finite; a program needn't handle non-finite values.
Results may differ from the reference program's by a relative error of at most 0.00166466.
Values are sent between devices in bfloat16 or wider.
A program may use at most 4.5 GiB of HBM per device.

```python
import jax
import jax.numpy as jnp
from jax import lax

D_MODEL = 4096
HEADS = 32
KV_HEADS = 8
HEAD = 128
FF = 14336
VOCAB = 32768
LAYERS = 2
WIDTH = 32
BEAMS = 32
SENTENCES = 1
SLOTS = 512

ROPE_BASE = 10000.0
NORM_EPS = 1e-6


def scaled_normal(key_in, shape, fan_in):
    return (jax.random.normal(key_in, shape, jnp.float32) * fan_in ** -0.5).astype(jnp.bfloat16)


def setup_inputs(seed: int = 0, part: int = 0) -> dict:
    base_key = jax.random.key(seed)
    shared = jax.random.split(base_key, 16)
    part_keys = jax.random.split(jax.random.fold_in(base_key, part), 16)
    position = jax.random.randint(shared[0], (1,), SLOTS // 2, SLOTS, dtype=jnp.int32)
    dominant = jnp.repeat(jax.random.randint(part_keys[0], (SENTENCES,), 0, WIDTH, dtype=jnp.int32), WIDTH)
    coin_flip = jax.random.randint(part_keys[1], (BEAMS,), 0, 2, dtype=jnp.int32)
    anyone = jax.random.randint(part_keys[2], (BEAMS,), 0, WIDTH, dtype=jnp.int32)
    first_beam = (jnp.arange(BEAMS, dtype=jnp.int32) // WIDTH) * WIDTH
    parent = (first_beam + jnp.where(coin_flip == 1, dominant, anyone)).reshape(SENTENCES, WIDTH)
    tok_emb = jax.random.normal(part_keys[3], (BEAMS, D_MODEL), jnp.float32).astype(jnp.bfloat16)
    beam_score = -6.0 * jax.random.uniform(part_keys[4], (BEAMS,), jnp.float32)
    late_slot = (jnp.arange(SLOTS) > position[0]).astype(jnp.float32)
    slot_amp = jax.random.normal(part_keys[5], (LAYERS, BEAMS, SLOTS), jnp.float32) + 2.0 * late_slot
    amp_b = slot_amp[:, :, :, None, None]
    key_dir = jax.random.normal(part_keys[6], (LAYERS, BEAMS, 1, KV_HEADS, HEAD), jnp.float32)
    val_dir = jax.random.normal(part_keys[7], (LAYERS, BEAMS, 1, KV_HEADS, HEAD), jnp.float32)
    cache_shape = (LAYERS, BEAMS, SLOTS, KV_HEADS, HEAD)
    k_cache = (1.5 * amp_b * key_dir + 0.5 * jax.random.normal(part_keys[8], cache_shape, jnp.float32)).astype(jnp.bfloat16)
    v_cache = (amp_b * val_dir + 0.5 * jax.random.normal(part_keys[9], cache_shape, jnp.float32)).astype(jnp.bfloat16)
    return {
        'tok_emb': tok_emb,
        'parent': parent,
        'position': position,
        'beam_score': beam_score,
        'k_cache': k_cache,
        'v_cache': v_cache,
        'w_query': scaled_normal(shared[1], (LAYERS, D_MODEL, HEADS * HEAD), D_MODEL),
        'w_key': scaled_normal(shared[2], (LAYERS, D_MODEL, KV_HEADS * HEAD), D_MODEL),
        'w_value': scaled_normal(shared[3], (LAYERS, D_MODEL, KV_HEADS * HEAD), D_MODEL),
        'w_out': scaled_normal(shared[4], (LAYERS, HEADS * HEAD, D_MODEL), HEADS * HEAD),
        'w_gate': scaled_normal(shared[5], (LAYERS, D_MODEL, FF), D_MODEL),
        'w_up': scaled_normal(shared[6], (LAYERS, D_MODEL, FF), D_MODEL),
        'w_down': scaled_normal(shared[7], (LAYERS, FF, D_MODEL), FF),
        'g_attn': jax.random.uniform(shared[8], (LAYERS, D_MODEL), jnp.float32, 0.5, 1.5).astype(jnp.bfloat16),
        'g_mlp': jax.random.uniform(shared[9], (LAYERS, D_MODEL), jnp.float32, 0.5, 1.5).astype(jnp.bfloat16),
        'g_final': jax.random.uniform(shared[10], (D_MODEL,), jnp.float32, 0.5, 1.5).astype(jnp.bfloat16),
        'w_vocab': (jax.random.normal(shared[11], (D_MODEL, VOCAB), jnp.float32) * 2.0 * D_MODEL ** -0.5).astype(jnp.bfloat16),
    }


def rms_norm(x_in, g_vec):
    mean_sq = jnp.mean(x_in * x_in, axis=-1, keepdims=True)
    return (x_in * lax.rsqrt(mean_sq + NORM_EPS) * g_vec.astype(jnp.float32)).astype(jnp.bfloat16)


def rope_at(x_in, cur_pos):
    half_dim = x_in.shape[-1] // 2
    inv_freq = ROPE_BASE ** (-2.0 * jnp.arange(half_dim, dtype=jnp.float32) / x_in.shape[-1])
    angles = cur_pos.astype(jnp.float32) * inv_freq
    cos_t = jnp.cos(angles)
    sin_t = jnp.sin(angles)
    x_f = x_in.astype(jnp.float32)
    x_lo = x_f[..., :half_dim]
    x_hi = x_f[..., half_dim:]
    rotated = jnp.concatenate([x_lo * cos_t - x_hi * sin_t, x_hi * cos_t + x_lo * sin_t], axis=-1)
    return rotated.astype(jnp.bfloat16)


def reference(tok_emb, parent, position, beam_score, k_cache, v_cache, w_query, w_key, w_value, w_out, w_gate, w_up, w_down, g_attn, g_mlp, g_final, w_vocab):
    cur_pos = position[0]
    q_groups = HEADS // KV_HEADS
    att_scale = HEAD ** -0.5
    flat_parent = parent.reshape(BEAMS)
    slot_valid = jnp.arange(SLOTS) <= cur_pos
    k_moved = jnp.take(k_cache, flat_parent, axis=1)
    v_moved = jnp.take(v_cache, flat_parent, axis=1)

    def layer_fn(residual, layer_in):
        k_lay, v_lay, wq_l, wk_l, wv_l, wo_l, wg_l, wu_l, wd_l, ga_l, gm_l = layer_in
        hidden = rms_norm(residual, ga_l)
        queries = rope_at(jnp.dot(hidden, wq_l, preferred_element_type=jnp.float32).astype(jnp.bfloat16).reshape(BEAMS, HEADS, HEAD), cur_pos)
        key_new = rope_at(jnp.dot(hidden, wk_l, preferred_element_type=jnp.float32).astype(jnp.bfloat16).reshape(BEAMS, 1, KV_HEADS, HEAD), cur_pos)
        val_new = jnp.dot(hidden, wv_l, preferred_element_type=jnp.float32).astype(jnp.bfloat16).reshape(BEAMS, 1, KV_HEADS, HEAD)
        k_lay = lax.dynamic_update_slice_in_dim(k_lay, key_new, cur_pos, axis=1)
        v_lay = lax.dynamic_update_slice_in_dim(v_lay, val_new, cur_pos, axis=1)
        q_grp = queries.reshape(BEAMS, KV_HEADS, q_groups, HEAD)
        scores = jnp.einsum('bkgd,bskd->bkgs', q_grp.astype(jnp.float32), k_lay.astype(jnp.float32)) * att_scale
        scores = jnp.where(slot_valid, scores, -jnp.inf)
        row_max = jnp.max(scores, axis=-1, keepdims=True)
        exp_scores = jnp.exp(scores - row_max)
        exp_total = jnp.sum(exp_scores, axis=-1)
        mix_sum = jnp.einsum('bkgs,bskd->bkgd', exp_scores.astype(jnp.bfloat16).astype(jnp.float32), v_lay.astype(jnp.float32))
        attn_out = (mix_sum / exp_total[..., None]).astype(jnp.bfloat16).reshape(BEAMS, HEADS * HEAD)
        residual = residual + jnp.dot(attn_out, wo_l, preferred_element_type=jnp.float32).astype(jnp.bfloat16).astype(jnp.float32)
        hidden = rms_norm(residual, gm_l)
        gate_act = jnp.dot(hidden, wg_l, preferred_element_type=jnp.float32).astype(jnp.bfloat16)
        up_act = jnp.dot(hidden, wu_l, preferred_element_type=jnp.float32).astype(jnp.bfloat16)
        swi_out = (jax.nn.silu(gate_act.astype(jnp.float32)) * up_act.astype(jnp.float32)).astype(jnp.bfloat16)
        residual = residual + jnp.dot(swi_out, wd_l, preferred_element_type=jnp.float32).astype(jnp.bfloat16).astype(jnp.float32)
        return residual, (k_lay, v_lay)

    layer_inputs = (k_moved, v_moved, w_query, w_key, w_value, w_out, w_gate, w_up, w_down, g_attn, g_mlp)
    residual, layer_caches = lax.scan(layer_fn, tok_emb.astype(jnp.float32), layer_inputs)
    k_out, v_out = layer_caches
    hidden = rms_norm(residual, g_final)
    logits = jnp.dot(hidden, w_vocab, preferred_element_type=jnp.float32)
    candidates = jnp.take(beam_score, flat_parent)[:, None] + jax.nn.log_softmax(logits, axis=-1)
    return (k_out, v_out, candidates)
```

```python
import functools

import jax
import jax.numpy as jnp
from jax import lax
from jax.experimental import pallas as pl
from jax.experimental.pallas import tpu as pltpu
from jax.sharding import PartitionSpec as P

ROPE_BASE, NORM_EPS, NEG = 10000.0, 1e-6, -1e30
MESH = pl.DeviceIdType.MESH
F32, BF16, I32 = jnp.float32, jnp.bfloat16, jnp.int32
G = 4
NB, NX, NA = 8, 16, 32
KVH, HD, HALF = 8, 128, 64
D, ROWS, SLOTS = 4096, 2048, 256
QW, KW, FW, VW = 1024, 256, 3584, 8192
QKV = QW + 2 * KW
NBUF = 12
TR, TC = 2048, 512
HT = 2
UT, UC = 7, 28
ONE, FIX = 1, 4
REST = NX - ONE - FIX
BUCKETS = (0, 1, 2, 3, 5, 7, 11)
SCALE = HD ** -0.5
EXP2 = SCALE * 1.4426950408889634
VM = pl.BlockSpec(memory_space=pltpu.VMEM)
HB = pl.BlockSpec(memory_space=pl.ANY)
SM = pl.BlockSpec(memory_space=pltpu.SMEM)
ROW = (ROWS, HD)
T_ORDER, T_START, T_COUNT, T_LIST, T_CODE, T_IDX, T_MISC, T_PAR = range(8)
DMA = pltpu.SemaphoreType.DMA


def coords():
    beam = lax.axis_index('beam')
    return beam // 2, lax.axis_index('sp'), beam % 2


def peer(x, y, c):
    return {'sp': y, 'beam': 2 * x + c}


def group_peers(x, y, c):
    return [(y, 1 - c), (1 - y, c), (1 - y, 1 - c)]


def all_peers(x, y, c):
    far = [(1 - x, yy, cc) for yy in (y, 1 - y) for cc in (c, 1 - c)]
    return far + [(x, yy, cc) for yy, cc in group_peers(x, y, c)]


def barrier_with(ids):
    sem = pltpu.get_barrier_semaphore()
    for dev in ids:
        pl.semaphore_signal(sem, inc=1, device_id=dev, device_id_type=MESH)
    pl.semaphore_wait(sem, len(ids))


def remote(src, dst, send_sem, recv_sem, dev):
    return pltpu.make_async_remote_copy(src_ref=src, dst_ref=dst, send_sem=send_sem, recv_sem=recv_sem,
                                        device_id=dev, device_id_type=MESH)


def local(src, dst, sem):
    return pltpu.make_async_copy(src, dst, sem)


def span(i, size):
    return pl.ds(pl.multiple_of(i * size, size), size)


def cols(i, size):
    return slice(i * size, (i + 1) * size)


def rsum(v):
    return jnp.sum(v, axis=-1, keepdims=True)


def rmax(v):
    return jnp.max(v, axis=-1, keepdims=True)


def csum(v):
    return jnp.sum(v, axis=0, keepdims=True)


def iota(shape_, dim):
    return lax.broadcasted_iota(I32, shape_, dim)


def mm(a, b):
    return jnp.dot(a, b, preferred_element_type=F32)


def start_all(copies):
    for cp in copies:
        cp.start()
    return copies


def wait_all(copies):
    for cp in copies:
        cp.wait()


class Stream:
    def __init__(self, wbuf, wsem, phases, ref_like):
        self.wbuf, self.wsem, self.like = wbuf, wsem, ref_like
        self.phases, base = [], 0
        for count, issue in phases:
            self.phases.append((base, count, issue))
            base += count
        self.total = base

    def issue(self, t, slot):
        for base, count, issue in self.phases:
            if isinstance(t, int):
                if base <= t < base + count:
                    issue(t - base, self.wbuf.at[slot], self.wsem.at[slot])
            else:
                @pl.when((t >= base) & (t < base + count))
                def _(base=base, issue=issue):
                    issue(t - base, self.wbuf.at[slot], self.wsem.at[slot])

    def prologue(self):
        for t in range(min(NBUF, self.total)):
            self.issue(t, t)

    def run(self, phase, body):
        base, count, _ = self.phases[phase]

        @pl.loop(0, count)
        def _(i):
            t = i + base
            slot = t % NBUF
            local(self.like, self.wbuf.at[slot], self.wsem.at[slot]).wait()
            body(i, self.wbuf.at[slot])
            self.issue(t + NBUF, slot)


def col_tiles(w_ref, layer, g, width, row_chunks):
    def issue(i, buf, sem):
        ci, ri = i // row_chunks, i % row_chunks
        at = pl.ds(pl.multiple_of(g * width + ci * TC, TC), TC)
        src = w_ref.at[span(ri, TR), at] if layer < 0 else w_ref.at[layer, span(ri, TR), at]
        local(src, buf, sem).start()
    return issue


def kv_tiles(wk_ref, wv_ref, layer, g):
    def issue(i, buf, sem):
        for k, w_ref in enumerate((wk_ref, wv_ref)):
            local(w_ref.at[layer, span(i, TR), span(g, KW)], buf.at[:, pl.ds(k * KW, KW)], sem).start()
    return issue


def gate_up_tiles(wg_ref, wu_ref, layer, g):
    def issue(i, buf, sem):
        at = pl.ds(pl.multiple_of(g * FW + (i // G) * TC, TC), TC)
        for k, w_ref in enumerate((wg_ref, wu_ref)):
            @pl.when((i // HT) % 2 == k)
            def _():
                local(w_ref.at[layer, span(i % HT, TR), at], buf, sem).start()
    return issue


def norm_into(r_ref, g_row, hbuf):
    total = rsum(r_ref[0] * r_ref[0])
    for k in range(1, G):
        total = total + rsum(r_ref[k] * r_ref[k])
    inv = lax.rsqrt(total / D + NORM_EPS)
    for k in range(G):
        gain = g_row[:, cols(k, QW)].astype(F32)
        hbuf[k // 2, :, cols(k % 2, QW)] = (r_ref[k] * inv * gain).astype(BF16)


def rope(x_bf, cos_row, sin_row):
    v = x_bf.astype(F32)
    return (v * cos_row + pltpu.roll(v, HALF, 1) * sin_row).astype(BF16)


def qkv_phases(stream, first, hbuf, acc, cos_row, sin_row, out_ref):
    acc[:] = jnp.zeros_like(acc)

    def body(i, w):
        acc[i // HT] += mm(hbuf[i % HT], w[:])

    def body_kv(i, w):
        acc[HT] += mm(hbuf[i], w[:])

    stream.run(first, body)
    stream.run(first + 1, body_kv)
    for head in range(QKV // HD):
        piece = acc[head // G, :, cols(head % G, HD)].astype(BF16)
        if head * HD < QW + KW:
            piece = rope(piece, cos_row, sin_row)
        out_ref[:, cols(head, HD)] = piece


def my_half(piece, c):
    wide = piece.astype(F32)
    return jnp.where(c == 0, wide[:NB], wide[NB:])


def spread_kv(buf, base, c, out_ref, at):
    for k in range(G):
        for j in range(G):
            part, h = j // 2, j % 2
            out_ref[:, at + part * KVH + 2 * k + h, :] = my_half(buf[base + k, :, QW + j * HD:QW + (j + 1) * HD], c)


def own_start(buf, g, sems, k0, peers, x):
    return start_all([remote(buf.at[g], buf.at[g], sems.at[0, k0, k], sems.at[1, k0, k], peer(x, *p))
                      for k, p in enumerate(peers)])


def kernel_table(par_ref, meta_ref):
    square = (NA, NA)
    i, j = iota(square, 0), iota(square, 1)
    par_row = jnp.broadcast_to(par_ref[:], square)
    par_col = rsum(jnp.where(i == j, par_row, 0).astype(F32)).astype(I32)
    fi, fj = i.astype(F32), j.astype(F32)

    def flag(v):
        return jnp.where(v, 1.0, 0.0)

    same, same_t = par_col == j, par_row == i
    far, half = (i // NX) != (j // NX), (i // NX) == (j // NX)
    before = rsum(flag((par_row < par_col) | ((par_row == par_col) & (j < i))))
    cross_row = jnp.minimum(csum(flag(same & far)), 1.0)
    cross_col = jnp.minimum(rsum(flag(same_t & far)), 1.0)
    place_col = rsum(flag(half & (j < i)) * cross_row)
    slot_col = place_col + (i // NX * NX).astype(F32)[:, :1]
    code = jnp.where(par_row // NB == j // NB, 0.0, jnp.where(par_row // NX == j // NX, 1.0, 2.0))[:1]
    place_par = csum(flag(same_t) * place_col)
    lane = j[:1]
    used = [rsum(jnp.where(lane // NX == k, cross_row, 0.0)) for k in range(2)]
    extra = jnp.maximum(used[0], used[1]) - (ONE + FIX)
    bucket = flag(extra > BUCKETS[0])
    for n in BUCKETS[1:]:
        bucket = bucket + flag(extra > n)
    misc = jnp.where(lane == 0, used[0], jnp.where(lane == 1, used[1], bucket))
    rows = [csum(jnp.where(before == fj, fi, 0.0)), csum(flag(par_col < j)), csum(flag(same)),
            csum(jnp.where(slot_col == fj, fi, 0.0) * cross_col), code,
            jnp.where(code > 1.0, place_par, (par_row % NB).astype(F32)[:1]), misc, par_row[:1].astype(F32)]
    for k, row in enumerate(rows):
        meta_ref[k:k + 1, :NA] = row.astype(I32)


def kernel_a(tok_ref, score_ref, cos_ref, sin_ref, ga_ref, wq_ref, wk_ref, wv_ref, k_ref, v_ref,
             q_out, kv_out, own_out, r_out, score_out, xp_out,
             wbuf, wsem, tokx, scx, r_s, hbuf, acc, qkvx, ssem, rsem, xsem):
    x, y, c = coords()
    g = y * 2 + c
    d = x * G + g
    stream = Stream(wbuf, wsem, [(G, col_tiles(wq_ref, 0, g, QW, HT)), (HT, kv_tiles(wk_ref, wv_ref, 0, g))],
                    wq_ref.at[0, pl.ds(0, TR), pl.ds(0, TC)])
    stream.prologue()
    others = all_peers(x, y, c)
    barrier_with([peer(*p) for p in others])
    tok_copy = remote(tok_ref, tokx, ssem.at[0], rsem.at[0], peer(x, y, 1 - c))
    tok_copy.start()
    beam = 2 * x + c
    sc_copies = start_all([remote(score_ref, scx.at[beam], ssem.at[k], rsem.at[k], peer(xx, y, cc))
                           for k, (xx, cc) in enumerate(((1 - x, c), (1 - x, 1 - c), (x, 1 - c)), 1)])
    scx[beam] = score_ref[:]
    for k in range(G):
        r_s[k, span(c, NB), :] = tok_ref[:, cols(k, QW)].astype(F32)
    tok_copy.wait()
    send_part(k_ref, v_ref, 1, 1 - c, xp_out, xsem, peer(x, y, 1 - c))
    for k in range(G):
        r_s[k, span(1 - c, NB), :] = tokx[:, cols(k, QW)].astype(F32)
    norm_into(r_s, ga_ref[0:1, :], hbuf)
    qkv_phases(stream, 0, hbuf, acc, cos_ref[:], sin_ref[:], qkvx.at[d])
    copies = start_all([remote(qkvx.at[d], qkvx.at[d], ssem.at[G + k], rsem.at[G + k], peer(*p))
                        for k, p in enumerate(others)])
    own_out[:] = qkvx[d]
    r_out[:] = r_s[:]
    wait_all(sc_copies)
    for k in range(G):
        score_out[cols(k, NB), :] = scx[k]
    wait_all(copies)
    for dd in range(2 * G):
        for h in range(KVH):
            q_out[cols(dd // G, NX), dd % G * KVH + h, :] = qkvx[dd, :, cols(h, HD)].astype(F32)
    spread_kv(qkvx, x * G, c, kv_out, 0)
    wait_part(xp_out, xsem, peer(x, y, 1 - c))


def send_part(k_ref, v_ref, layer, part, out, xsem, dev):
    for k, ref in enumerate((k_ref, v_ref)):
        @pl.when(part == k)
        def _():
            @pl.loop(0, NB)
            def _(r):
                remote(ref.at[layer, r], out.at[r], xsem.at[0], xsem.at[1], dev).start()


def wait_part(out, xsem, dev):
    remote(out, out, xsem.at[0], xsem.at[1], dev).wait()


def mask_bias(limit):
    row, col = iota((NA, ROWS), 0), iota((NA, ROWS), 1)
    ok = ((col % KVH) == (row // G)) & (col < limit * KVH)
    return jnp.where(ok, 0.0, NEG)


def attend(q, k_rows, v_rows, bias):
    s = lax.dot_general(q, k_rows, (((1,), (1,)), ((), ())), preferred_element_type=F32)
    s = (s.reshape(-1, NA, ROWS) + bias[:]).reshape(s.shape)
    m = rmax(s)
    e = jnp.exp2((s - m) * EXP2)
    return mm(e.astype(BF16), v_rows), m * SCALE, rsum(e)


def to_lanes(column):
    return csum(jnp.where(iota((NA, HD), 0) == iota((NA, HD), 1), column, 0.0))


def keep(o_ref, st_ref, b, o, m, total):
    o_ref[b] = o
    st_ref[0, pl.ds(b, 1), :] = to_lanes(m)
    st_ref[1, pl.ds(b, 1), :] = to_lanes(total)


def kernel_home(meta, pos_ref, q_ref, k_ref, v_ref, o_ref, st_ref, kbuf, vbuf, bias, ksem, vsem):
    x, y, c = coords()
    first = (2 * x + c) * NB
    limit = jnp.clip(pos_ref[0] - y * SLOTS, 0, SLOTS)

    def count_of(r):
        return jnp.where(limit > 0, meta[T_COUNT, first + r], 0)

    def copies(r):
        return local(k_ref.at[0, r], kbuf.at[r], ksem.at[r]), local(v_ref.at[0, r], vbuf.at[r], vsem.at[r])

    @pl.loop(0, NB)
    def _(r):
        @pl.when(count_of(r) > 0)
        def _():
            start_all(copies(r))

    o_ref[:] = jnp.zeros_like(o_ref)
    st_ref[0] = jnp.full((NA, HD), NEG, F32)
    st_ref[1] = jnp.zeros((NA, HD), F32)
    bias[:] = mask_bias(limit)

    @pl.loop(0, NB)
    def _(r):
        count = count_of(r)
        start = meta[T_START, first + r]

        @pl.when(count > 0)
        def _():
            wait_all(copies(r))

        def step(s, carry):
            beams = [meta[T_ORDER, start + jnp.minimum(s * G + j, count - 1)] for j in range(G)]
            q = jnp.concatenate([q_ref[b] for b in beams], axis=0).astype(BF16)
            o, m, total = attend(q, kbuf[r], vbuf[r], bias)
            for j, b in enumerate(beams):
                at = cols(j, NA)
                keep(o_ref, st_ref, b, o[at], m[at], total[at])
            return carry

        lax.fori_loop(0, (count + G - 1) // G, step, 0)


def lane_pick(rows, lane):
    return rsum(jnp.where(iota(rows.shape, 1) == lane, rows, 0.0))


def kernel_c(o_ref, st_ref, own_ref, out_ref, ox, sx, ssem, rsem):
    x, y, c = coords()
    g = y * 2 + c
    d = x * G + g
    others = all_peers(x, y, c)
    barrier_with([peer(*p) for p in others])
    copies = []
    for k, (xx, yy, cc) in enumerate(others):
        beams, heads, dev = span(xx, NX), span(yy * 2 + cc, KVH), peer(xx, yy, cc)
        copies.append(remote(st_ref.at[:, beams, :], sx.at[d], ssem.at[0, k], rsem.at[0, k], dev))
        copies.append(remote(o_ref.at[beams, heads, :], ox.at[d], ssem.at[1, k], rsem.at[1, k], dev))
    start_all(copies)
    sx[d] = st_ref[:, span(x, NX), :]
    ox[d] = o_ref[span(x, NX), span(g, KVH), :]
    lanes = iota((NX, HD), 1)
    s_self = jnp.full((NX, HD), NEG, F32)
    for h in range(KVH):
        q = own_ref[:, cols(h, HD)].astype(F32)
        kk = own_ref[:, cols(KVH + h // G, HD)].astype(F32)
        s_self = jnp.where(lanes == g * KVH + h, rsum(q * kk) * SCALE, s_self)
    wait_all(copies)
    top = s_self
    for i in range(2 * G):
        top = jnp.maximum(top, sx[i, 0])
    e_self = jnp.exp(s_self - top)
    total = e_self
    weights = []
    for i in range(2 * G):
        weights.append(jnp.exp(sx[i, 0] - top))
        total = total + weights[i] * sx[i, 1]
    for h in range(KVH):
        lane = g * KVH + h
        vv = own_ref[:, cols(KVH + 2 + h // G, HD)].astype(F32)
        mix = lane_pick(e_self, lane).astype(BF16).astype(F32) * vv
        for i in range(2 * G):
            mix = mix + lane_pick(weights[i], lane) * ox[i, :, h, :]
        out_ref[:, cols(h, HD)] = (mix / lane_pick(total, lane)).astype(BF16)


class Crossing:
    def __init__(self, x, y, c, rows, sems):
        self.first, self.second = [], []
        for k, (src, got, passed) in enumerate(rows):
            if src is not got:
                self.first.append(remote(src, got, sems.at[0, k], sems.at[1, k], peer(1 - x, y, c)))
            self.second.append(remote(got, passed, sems.at[2, k], sems.at[3, k], peer(x, y, 1 - c)))
        self.ready = len(self.second) - len(self.first)

    def start(self):
        start_all(self.first)
        start_all(self.second[:self.ready])

    def forward(self, k):
        self.first[k].wait_recv()
        self.second[self.ready + k].start()

    def finish(self, k):
        for i in range(k, len(self.first)):
            self.forward(i)
        for cp in self.first:
            cp.wait_send()
        wait_all(self.second)


def out_mlp(stream, first, g, x, peers, r_s, hbuf, acc, ox, yx, zx, ubuf, gacc, gm_row, sems, usem, cross, side):
    def add(buf):
        for k in range(G):
            r_s[k] = r_s[k] + buf[k].astype(F32)

    def send_acc(buf, k0):
        for k in range(HT):
            buf[g, :, cols(k, TC)] = acc[k].astype(BF16)
        wait_all(own_start(buf, g, sems, k0, peers, x))
        add(buf)

    copies = own_start(ox, g, sems, 0, peers, x)
    cross.start()
    acc[:] = jnp.zeros_like(acc)
    wait_all(copies)
    for k in range(G):
        hbuf[k // 2, :, cols(k % 2, QW)] = ox[k]

    def body_out(i, w):
        acc[i // HT] += mm(hbuf[i % HT], w[:])

    stream.run(first, body_out)
    send_acc(yx, 1)
    norm_into(r_s, gm_row, hbuf)

    def body_gu(i, w):
        part, ri = (i // HT) % 2, i % HT
        side(i)
        part_sum = mm(hbuf[ri], w[:])

        @pl.when(ri == 0)
        def _():
            gacc[part] = part_sum

        @pl.when(ri == 1)
        def _():
            gacc[part] += part_sum

        @pl.when(i % G == G - 1)
        def _():
            at = g * UT + i // G
            gate = gacc[0].astype(BF16).astype(F32)
            up = gacc[1].astype(BF16).astype(F32)
            ubuf[at] = (jax.nn.silu(gate) * up).astype(BF16)
            start_all([remote(ubuf.at[at], ubuf.at[at], usem.at[0, k], usem.at[1, k], peer(x, *p))
                       for k, p in enumerate(peers)])

    stream.run(first + 1, body_gu)
    acc[:] = jnp.zeros_like(acc)
    cross.forward(0)
    mine = ubuf.at[pl.ds(g * UT, UT)]
    wait_all([remote(mine, mine, usem.at[0, k], usem.at[1, k], peer(x, *p)) for k, p in enumerate(peers)])

    def body_down(i, w):
        ci, ri = i // UT, i % UT
        total = mm(ubuf[G * ri], w[cols(0, TC), :])
        for k in range(1, G):
            total = total + mm(ubuf[G * ri + k], w[cols(k, TC), :])
        acc[ci] += total

    stream.run(first + 2, body_down)
    send_acc(zx, 2)


def mlp_phases(layer, g, wo_ref, wg_ref, wu_ref, wd_ref):
    return [(G, col_tiles(wo_ref, layer, g, QW, HT)),
            (UC, gate_up_tiles(wg_ref, wu_ref, layer, g)),
            (2 * UT, col_tiles(wd_ref, layer, g, QW, UT))]


def kernel_mid(o_ref, r_ref, cos_ref, sin_ref, ga_ref, gm_ref, wo_ref, wg_ref, wu_ref, wd_ref, wq_ref, wk_ref, wv_ref,
               k_ref, v_ref, one_ref, fix_ref,
               qkv_out, r_out, one_p, fix_r, fix_p, xq_out, kp_out, vp_out,
               wbuf, wsem, r_s, hbuf, acc, ox, yx, zx, ubuf, gacc, qkvx, sems, usem, csem, xsem):
    x, y, c = coords()
    g = y * 2 + c
    peers = group_peers(x, y, c)
    stream = Stream(wbuf, wsem, mlp_phases(0, g, wo_ref, wg_ref, wu_ref, wd_ref) + [
        (G, col_tiles(wq_ref, 1, g, QW, HT)), (HT, kv_tiles(wk_ref, wv_ref, 1, g))],
        wq_ref.at[0, pl.ds(0, TR), pl.ds(0, TC)])
    stream.prologue()
    beside = peer(x, y, 1 - c)
    barrier_with([peer(x, *p) for p in peers] + [peer(1 - x, y, c)])
    here = one_ref.at[0]
    rows = [(here, here, one_p.at[0])] + [(fix_ref.at[k], fix_r.at[k], fix_p.at[k]) for k in range(FIX)]
    cross = Crossing(x, y, c, rows, csem)
    ox[g] = o_ref[:]
    r_s[:] = r_ref[:]

    def side(i):
        r, which = i % NB, i // NB
        for k, ref in enumerate((k_ref, v_ref)):
            @pl.when((which == 0) & (c == k))
            def _():
                remote(ref.at[1, r], xq_out.at[r], xsem.at[0, 0], xsem.at[1, 0], beside).start()
        for k, (ref, out) in enumerate(((k_ref, kp_out), (v_ref, vp_out)), 1):
            @pl.when(which == k)
            def _():
                remote(ref.at[0, r], out.at[r], xsem.at[0, k], xsem.at[1, k], beside).start()

    out_mlp(stream, 0, g, x, peers, r_s, hbuf, acc, ox, yx, zx, ubuf, gacc, gm_ref[0:1, :], sems, usem, cross, side)
    cross.forward(1)
    norm_into(r_s, ga_ref[1:2, :], hbuf)
    qkv_phases(stream, 3, hbuf, acc, cos_ref[:], sin_ref[:], qkvx.at[g])
    copies = own_start(qkvx, g, sems, 3, peers, x)
    cross.forward(2)
    r_out[:] = r_s[:]
    for k, out in enumerate((xq_out, kp_out, vp_out)):
        remote(out, out, xsem.at[0, k], xsem.at[1, k], beside).wait()
    wait_all(copies)
    for k in range(G):
        for h in range(KVH):
            qkv_out[:, k * KVH + h, :] = my_half(qkvx[k, :, cols(h, HD)], c)
    spread_kv(qkvx, 0, c, qkv_out, NA)
    cross.finish(3)


def kernel_end(o_ref, st_ref, r_ref, score_ref, gm_ref, gf_ref, wo_ref, wg_ref, wu_ref, wd_ref, wvoc_ref,
               one_ref, fix_ref,
               cand_ref, one_r, one_p, fix_r, fix_p,
               wbuf, wsem, r_s, hbuf, acc, ox, yx, zx, ubuf, gacc, px, sx, lacc, lbuf, candx, stx, run_st,
               sems, usem, psem, lsem, csem):
    x, y, c = coords()
    g = y * 2 + c
    peers = group_peers(x, y, c)
    stream = Stream(wbuf, wsem, mlp_phases(1, g, wo_ref, wg_ref, wu_ref, wd_ref) + [
        (VW // TC * HT, col_tiles(wvoc_ref, -1, g, VW, HT))],
        wvoc_ref.at[pl.ds(0, TR), pl.ds(0, TC)])
    stream.prologue()
    barrier_with([peer(x, *p) for p in peers] + [peer(1 - x, y, c)])
    rows = [(one_ref.at[0], one_r.at[0], one_p.at[0])] + [(fix_ref.at[k], fix_r.at[k], fix_p.at[k]) for k in range(FIX)]
    cross = Crossing(x, y, c, rows, csem)
    copies = []
    for k, (yy, cc) in enumerate(peers):
        heads, dev = span(yy * 2 + cc, KVH), peer(x, yy, cc)
        copies.append(remote(st_ref, sx.at[g], psem.at[0, 0, k], psem.at[1, 0, k], dev))
        copies.append(remote(o_ref.at[:, heads, :], px.at[g], psem.at[0, 1, k], psem.at[1, 1, k], dev))
    start_all(copies)
    sx[g] = st_ref[:]
    px[g] = o_ref[:, span(g, KVH), :]
    r_s[:] = r_ref[:]
    wait_all(copies)
    for cc in range(2):
        pair = (cc, 2 + cc)
        top = jnp.maximum(sx[pair[0], 0], sx[pair[1], 0])
        weights = [jnp.exp(sx[p, 0] - top) for p in pair]
        total = weights[0] * sx[pair[0], 1] + weights[1] * sx[pair[1], 1]
        for h in range(KVH):
            lane = g * KVH + h
            mix = lane_pick(weights[0], lane) * px[pair[0], :, h, :] + lane_pick(weights[1], lane) * px[pair[1], :, h, :]
            acc[h // G, cols(cc, NB), cols(h % G, HD)] = mix / lane_pick(total, lane)
    for k in range(HT):
        ox[g, :, cols(k, TC)] = acc[k].astype(BF16)
    out_mlp(stream, 0, g, x, peers, r_s, hbuf, acc, ox, yx, zx, ubuf, gacc, gm_ref[1:2, :], sems, usem, cross, lambda i: i)
    cross.forward(1)
    norm_into(r_s, gf_ref[:], hbuf)
    run_st[0] = jnp.full((NX, HD), NEG, F32)
    run_st[1] = jnp.zeros((NX, HD), F32)
    nv = VW // TC

    def body_voc(i, w):
        ci, ri = i // HT, i % HT
        part_sum = mm(hbuf[ri], w[:])

        @pl.when(ri == 0)
        def _():
            lacc[:] = part_sum

        @pl.when(ri == 1)
        def _():
            logits = lacc[:] + part_sum
            for cc in range(2):
                lbuf[ci, cc] = logits[cols(cc, NB)]
            at = g * nv + ci
            candx[at] = lbuf[ci, c]
            start_all([remote(lbuf.at[ci, cc], candx.at[at], lsem.at[0, k], lsem.at[1, k], peer(x, yy, cc))
                       for k, (yy, cc) in enumerate(peers)])
            old = run_st[0][:, :1]
            top = jnp.maximum(old, rmax(logits))
            run_st[1] = run_st[1] * jnp.exp(old - top) + rsum(jnp.exp(logits - top))
            run_st[0] = jnp.broadcast_to(top, (NX, HD))

    stream.run(3, body_voc)
    stx[g] = run_st[:]
    wait_all(own_start(stx, g, sems, 3, peers, x))
    tops = [stx[k, 0, span(c, NB), :] for k in range(G)]
    top = functools.reduce(jnp.maximum, tops)
    total = sum(stx[k, 1, span(c, NB), :] * jnp.exp(tops[k] - top) for k in range(G))
    log_z = top + jnp.log(total)
    score = score_ref[:]
    got = candx.at[pl.ds(g * nv, nv)]
    wait_all([remote(lbuf.at[:, cc], got, lsem.at[0, k], lsem.at[1, k], peer(x, yy, cc)) for k, (yy, cc) in enumerate(peers)])

    @pl.loop(0, G * nv)
    def _(i):
        cand_ref[:, span(i, TC)] = score[:, :1] + (candx[i] - log_z[:, :1])

    cross.finish(2)


def kernel_pack(layer, meta, dep, k_ref, v_ref, xk_ref, xv_ref, one, fix, rest, buf, isem, osem):
    x, y, c = coords()
    count = meta[T_MISC, x]
    segments = ((one, 0, ONE), (fix, ONE, ONE + FIX), (rest, ONE + FIX, NX))

    def fetch(p):
        v = meta[T_LIST, x * NX + p]
        r, own = v % NB, (v // NB) % 2 == c
        for core, mine, theirs in ((0, k_ref, xk_ref), (1, v_ref, xv_ref)):
            @pl.when((c == core) & own)
            def _():
                local(mine.at[layer, r], buf.at[p], isem.at[p]).start()

            @pl.when((c == core) & jnp.logical_not(own))
            def _():
                local(theirs.at[r], buf.at[p], isem.at[p]).start()

    def store(p, op):
        for ref, lo, hi in segments:
            @pl.when((p >= lo) & (p < hi))
            def _():
                op(local(buf.at[p], ref.at[jnp.clip(p - lo, 0, hi - lo - 1)], osem.at[p]))

    def each(fn):
        lax.fori_loop(0, count, lambda p, z: (fn(p), z)[1], 0)

    def move(p):
        local(xk_ref.at[0], buf.at[p], isem.at[p]).wait()
        store(p, lambda cp: cp.start())

    each(fetch)
    each(move)
    each(lambda p: store(p, lambda cp: cp.wait()))


def fetch_row(layer, meta, b, mine, own_ref, partner, crossed, dst, sem):
    code, idx = meta[T_CODE, b], meta[T_IDX, b]

    @pl.when(code == 0)
    def _():
        local(own_ref.at[layer, idx % NB], dst, sem).start()

    for ref, cond in zip(partner, (mine, jnp.logical_not(mine))):
        @pl.when((code == 1) & cond)
        def _():
            local(ref.at[idx % NB], dst, sem).start()

    for lo, hi, refs in crossed:
        for ref, cond in zip(refs, (mine, jnp.logical_not(mine))):
            @pl.when((code == 2) & (idx >= lo) & (idx < hi) & cond)
            def _():
                local(ref.at[jnp.clip(idx - lo, 0, hi - lo - 1)], dst, sem).start()


def put_new(buf, i, new, at):
    rows = span(at // 2, NX)
    hit = iota((NX, HD), 0) // KVH == at % 2
    both = jnp.concatenate([new, new], axis=0)
    buf[i, rows, :] = jnp.where(hit, both, buf[i, rows, :].astype(F32)).astype(BF16)


def kernel_child(layer, *refs):
    if layer:
        (meta, pos_ref, new_ref, score_ref, k_ref, v_ref, xp, xq, *moved,
         ko, vo, o_ref, st_ref, score_out, kbuf, vbuf, isem, osem, bias) = refs
        partners, at0 = ((xp, xq), (xp, xq)), NA
    else:
        (meta, pos_ref, new_ref, k_ref, v_ref, kp, vp, *moved, _, _,
         ko, vo, kbuf, vbuf, isem, osem) = refs
        partners, at0 = ((kp, kp), (vp, vp)), 0
    x, y, c = coords()
    first = (2 * x + c) * NB
    pos = pos_ref[0] - y * SLOTS
    one_r, one_p, fix_r, fix_p, rest_r, rest_p = moved
    crossed = ((0, ONE, (one_r, one_p)), (ONE, ONE + FIX, (fix_r, fix_p)), (ONE + FIX, NX, (rest_r, rest_p)))
    both = ((k_ref, kbuf, ko), (v_ref, vbuf, vo))

    @pl.loop(0, NB)
    def _(i):
        for part, (src, buf, _) in enumerate(both):
            fetch_row(layer, meta, first + i, c == part, src, partners[part], crossed, buf.at[i], isem.at[part, i])

    if layer:
        bias[:] = mask_bias(jnp.clip(pos + 1, 1, SLOTS))

    @pl.loop(0, NB)
    def _(i):
        for part, (src, buf, out) in enumerate(both):
            local(src.at[0, 0], buf.at[i], isem.at[part, i]).wait()

            @pl.when((pos >= 0) & (pos < SLOTS))
            def _():
                start = at0 + part * KVH
                put_new(buf, i, new_ref[i, start:start + KVH, :], jnp.clip(pos, 0, SLOTS - 1))

            local(buf.at[i], out.at[layer, i], osem.at[part, i]).start()
        if layer:
            keep(o_ref, st_ref, i, *attend(new_ref[i, :NA, :].astype(BF16), kbuf[i], vbuf[i], bias))
            score_out[pl.ds(i, 1), :] = score_ref[pl.ds(meta[T_PAR, first + i], 1), :]

    @pl.loop(0, NB)
    def _(i):
        for part, (_, buf, out) in enumerate(both):
            local(buf.at[i], out.at[layer, i], osem.at[part, i]).wait()


def kernel_rest(n, src, got, passed, sems):
    x, y, c = coords()
    barrier_with([peer(1 - x, y, c), peer(x, y, 1 - c)])
    cross = Crossing(x, y, c, [(src.at[i], got.at[i], passed.at[i]) for i in range(n)], sems)
    cross.start()
    cross.finish(0)


def shape(s, t=BF16):
    return jax.ShapeDtypeStruct(s, t)


def rows_of(n):
    return shape((n,) + ROW)


def scratch_stream():
    return [pltpu.VMEM((NBUF, TR, TC), BF16), DMA((NBUF,))]


def scratch_mlp():
    wide = (G, NX, QW)
    return [pltpu.VMEM(wide, F32), pltpu.VMEM((HT, NX, TR), BF16), pltpu.VMEM((HT + 1, NX, TC), F32),
            pltpu.VMEM(wide, BF16), pltpu.VMEM(wide, BF16), pltpu.VMEM(wide, BF16),
            pltpu.VMEM((UC, NX, TC), BF16), pltpu.VMEM((HT, NX, TC), F32)]


def call(kernel, name, us, outs, ins, scratch, cid=-1, aliases=()):
    more = {} if cid < 0 else dict(collective_id=cid, has_side_effects=True)
    return pl.pallas_call(
        kernel, out_shape=tuple(o for o, _ in outs), in_specs=ins, out_specs=tuple(s for _, s in outs),
        scratch_shapes=scratch, input_output_aliases=dict(aliases), name=name,
        cost_estimate=pl.CostEstimate(flops=us * 400000000, bytes_accessed=us * 3000000, transcendentals=0),
        compiler_params=pltpu.CompilerParams(vmem_limit_bytes=59 * 2 ** 20, **more))


def solution(mesh):
    beam_spec = P(('dp', 'beam'))
    row_spec = P(('dp', 'beam'), None)
    cache_spec = P(None, ('dp', 'beam'), 'sp', None, None)
    full_rep = P()
    swap_x = [(b, (b + 2) % G) for b in range(G)]

    def rest(index, packed):
        def branch(k, n):
            outs = [(rows_of(REST), HB)] * 2
            if n == 0:
                return call(lambda *_: None, 'rest_none', 1, outs, [HB], [])
            return call(functools.partial(kernel_rest, n), f'rest_{n}', 1, outs, [HB], [DMA((4, n))], NB + k)
        return lax.switch(index, [branch(k, n) for k, n in enumerate(BUCKETS)], packed)

    def local_step(tok_emb, parent, position, beam_score, k_cache, v_cache, w_query, w_key, w_value, w_out, w_gate, w_up, w_down, g_attn, g_mlp, g_final, w_vocab):
        cur_pos = position[0]
        half = jnp.arange(HD, dtype=I32) % HALF
        inv_freq = ROPE_BASE ** (-2.0 * half.astype(F32) / HD)
        angles = (cur_pos.astype(F32) * inv_freq)[None, :]
        cos_row = jnp.cos(angles)
        sin_row = jnp.sin(angles) * jnp.where(jnp.arange(HD) < HALF, -1.0, 1.0)
        kc, vc = k_cache.reshape((2, NB) + ROW), v_cache.reshape((2, NB) + ROW)
        score_in = jnp.broadcast_to(beam_score[:, None], (NB, HD))
        lanes = shape((NA, HD), F32)

        meta, = call(kernel_table, 'table', 2, [(shape((NB, HD), I32), VM)], [VM], [])(parent)
        bucket = meta[T_MISC, 2]

        q0, kv0, own0, r0, scores, xp1 = call(
            kernel_a, 'qkv_first', 12,
            [(shape((NA, NA, HD), F32), VM), (shape((NB, NX, HD), F32), VM), (shape((NX, QKV)), VM),
             (shape((G, NX, QW), F32), VM), (lanes, VM), (rows_of(NB), HB)],
            [VM] * 5 + [HB] * 5,
            scratch_stream() + [
                pltpu.VMEM((NB, D), BF16), pltpu.VMEM((G, NB, HD), F32), pltpu.VMEM((G, NX, QW), F32),
                pltpu.VMEM((HT, NX, TR), BF16), pltpu.VMEM((HT + 1, NX, TC), F32), pltpu.VMEM((2 * G, NX, QKV), BF16),
                DMA((3 * G,)), DMA((3 * G,)), DMA((2,))], 1,
        )(tok_emb, score_in, cos_row, sin_row, g_attn, w_query, w_key, w_value, kc, vc)

        def pack_rows(layer, dep, xk, xv):
            return call(functools.partial(kernel_pack, layer), f'pack_{layer}', 3,
                        [(rows_of(ONE), HB), (rows_of(FIX), HB), (rows_of(REST), HB)], [SM] + [HB] * 5,
                        [pltpu.VMEM((NX,) + ROW, BF16), DMA((NX,)), DMA((NX,))])(meta, dep, kc, vc, xk, xv)

        one1, fix1, rest1 = pack_rows(1, own0, xp1, xp1)
        one_r1 = lax.ppermute(one1, 'beam', swap_x)

        o0, st0 = call(
            kernel_home, 'attend_home', 9, [(shape((NA, NA, HD), F32), VM), (shape((2, NA, HD), F32), VM)],
            [SM, SM, VM, HB, HB],
            [pltpu.VMEM((NB,) + ROW, BF16)] * 2 + [pltpu.VMEM((NA, ROWS), F32), DMA((NB,)), DMA((NB,))],
        )(meta, position, q0, kc, vc)
        o0, one_r1 = lax.optimization_barrier((o0, one_r1))

        o_mine, = call(
            kernel_c, 'combine_first', 9, [(shape((NX, QW)), VM)], [VM] * 3,
            [pltpu.VMEM((2 * G, NX, KVH, HD), F32), pltpu.VMEM((2 * G, 2, NX, HD), F32), DMA((2, 7)), DMA((2, 7))], 2,
        )(o0, st0, own0)

        weights = (w_out, w_gate, w_up, w_down)
        qkv1, r1, one_p1, fix_r1, fix_p1, xq1, kp0, vp0 = call(
            kernel_mid, 'mlp_first', 45,
            [(shape((NB, NA + NX, HD), F32), VM), (shape((G, NX, QW), F32), VM), (rows_of(ONE), HB),
             (rows_of(FIX), HB), (rows_of(FIX), HB), (rows_of(NB), HB), (rows_of(NB), HB), (rows_of(NB), HB)],
            [VM] * 6 + [HB] * 11,
            scratch_stream() + scratch_mlp() + [pltpu.VMEM((G, NX, QKV), BF16), DMA((2, G, 3)), DMA((2, 3)), DMA((4, ONE + FIX)), DMA((2, 3))], 3,
        )(o_mine, r0, cos_row, sin_row, g_attn, g_mlp, *weights, w_query, w_key, w_value, kc, vc, one_r1, fix1)

        one0, fix0, rest0 = pack_rows(0, r1, kp0, vp0)
        rest1, _ = lax.optimization_barrier((rest1, r1))
        rest_r1, rest_p1 = rest(bucket, rest1)

        child_scratch = [pltpu.VMEM((NB,) + ROW, BF16), pltpu.VMEM((NB,) + ROW, BF16), DMA((2, NB)), DMA((2, NB))]
        cache_out = [(shape((2, NB) + ROW), HB)] * 2
        ko, vo, o1, st1, score1 = call(
            functools.partial(kernel_child, 1), 'attend_child', 9,
            cache_out + [(shape((NB, NA, HD), F32), VM), (shape((2, NB, HD), F32), VM), (shape((NB, HD), F32), VM)],
            [SM, SM, VM, VM] + [HB] * 10, child_scratch + [pltpu.VMEM((NA, ROWS), F32)],
        )(meta, position, qkv1, scores, kc, vc, xp1, xq1, one_r1, one_p1, fix_r1, fix_p1, rest_r1, rest_p1)

        cand, one_r0, one_p0, fix_r0, fix_p0 = call(
            kernel_end, 'mlp_vocab', 58,
            [(shape((NB, G * VW), F32), VM), (rows_of(ONE), HB), (rows_of(ONE), HB), (rows_of(FIX), HB), (rows_of(FIX), HB)],
            [VM] * 6 + [HB] * 7,
            scratch_stream() + scratch_mlp() + [
                pltpu.VMEM((G, NB, KVH, HD), F32), pltpu.VMEM((G, 2, NB, HD), F32), pltpu.VMEM((NX, TC), F32),
                pltpu.VMEM((VW // TC, 2, NB, TC), F32), pltpu.VMEM((G * VW // TC, NB, TC), F32), pltpu.VMEM((G, 2, NX, HD), F32),
                pltpu.VMEM((2, NX, HD), F32),
                DMA((2, G, 3)), DMA((2, 3)), DMA((2, 2, 3)), DMA((2, 3)), DMA((4, ONE + FIX))], 4,
        )(o1, st1, r1, score1, g_mlp, g_final[None, :], *weights, w_vocab, one0, fix0)

        rest0, cand = lax.optimization_barrier((rest0, cand))
        rest_r0, rest_p0 = rest(bucket, rest0)
        ko, vo = call(
            functools.partial(kernel_child, 0), 'assemble_first', 8, cache_out, [SM, SM, VM] + [HB] * 12, child_scratch,
            -1, ((13, 0), (14, 1)),
        )(meta, position, kv0, kc, vc, kp0, vp0, one_r0, one_p0, fix_r0, fix_p0, rest_r0, rest_p0, ko, vo)
        return ko.reshape(k_cache.shape), vo.reshape(v_cache.shape), cand

    in_specs = (row_spec, P('dp', None), full_rep, beam_spec, cache_spec, cache_spec) + (full_rep,) * 11
    return jax.shard_map(local_step, mesh=mesh, in_specs=in_specs, out_specs=(cache_spec, cache_spec, row_spec), check_vma=False)
```

```python
import functools

import jax
import jax.numpy as jnp
from jax import lax
from jax.experimental import pallas as pl
from jax.experimental.pallas import tpu as pltpu
from jax.sharding import PartitionSpec as P

ROPE_BASE, NORM_EPS, NEG = 10000.0, 1e-6, -1e30
MESH = pl.DeviceIdType.MESH
F32, BF16, I32 = jnp.float32, jnp.bfloat16, jnp.int32
G = 4
NB, NX, NA = 8, 16, 32
KVH, HD, HALF = 8, 128, 64
D, ROWS, SLOTS = 4096, 2048, 256
QW, KW, FW, VW = 1024, 256, 3584, 8192
QKV = QW + 2 * KW
FEW, MANY = 6, 20
TR, TC = 2048, 512
HT = 2
UT, UC = 7, 28
ONE, FIXES = 1, (3, 4, 5)
FIX = FIXES[-1]
REST = NX - ONE - FIX
BUCKETS = (0, 1, 2, 4, 10)
SCALE = HD ** -0.5
EXP2 = SCALE * 1.4426950408889634
VM = pl.BlockSpec(memory_space=pltpu.VMEM)
HB = pl.BlockSpec(memory_space=pl.ANY)
SM = pl.BlockSpec(memory_space=pltpu.SMEM)
ROW = (ROWS, HD)
T_ORDER, T_START, T_COUNT, T_LIST, T_CODE, T_IDX, T_MISC, T_PAR = range(8)
DMA = pltpu.SemaphoreType.DMA


def coords():
    beam = lax.axis_index('beam')
    return beam // 2, lax.axis_index('sp'), beam % 2


def peer(x, y, c):
    return {'sp': y, 'beam': 2 * x + c}


def group_peers(x, y, c):
    return [(y, 1 - c), (1 - y, c), (1 - y, 1 - c)]


def all_peers(x, y, c):
    far = [(1 - x, yy, cc) for yy in (y, 1 - y) for cc in (c, 1 - c)]
    return far + [(x, yy, cc) for yy, cc in group_peers(x, y, c)]


def barrier_with(ids):
    sem = pltpu.get_barrier_semaphore()
    for dev in ids:
        pl.semaphore_signal(sem, inc=1, device_id=dev, device_id_type=MESH)
    pl.semaphore_wait(sem, len(ids))


def remote(src, dst, send_sem, recv_sem, dev):
    return pltpu.make_async_remote_copy(src_ref=src, dst_ref=dst, send_sem=send_sem, recv_sem=recv_sem,
                                        device_id=dev, device_id_type=MESH)


def local(src, dst, sem):
    return pltpu.make_async_copy(src, dst, sem)


def span(i, size):
    return pl.ds(pl.multiple_of(i * size, size), size)


def cols(i, size):
    return slice(i * size, (i + 1) * size)


def rsum(v):
    return jnp.sum(v, axis=-1, keepdims=True)


def rmax(v):
    return jnp.max(v, axis=-1, keepdims=True)


def csum(v):
    return jnp.sum(v, axis=0, keepdims=True)


def iota(shape_, dim):
    return lax.broadcasted_iota(I32, shape_, dim)


def mm(a, b):
    return jnp.dot(a, b, preferred_element_type=F32)


def start_all(copies):
    for cp in copies:
        cp.start()
    return copies


def wait_all(copies):
    for cp in copies:
        cp.wait()


class Stream:
    def __init__(self, wbuf, wsem, phases, ref_like):
        self.wbuf, self.wsem, self.like, self.depth = wbuf, wsem, ref_like, wbuf.shape[0]
        self.phases, base = [], 0
        for count, issue in phases:
            self.phases.append((base, count, issue))
            base += count
        self.total = base

    def issue(self, t, slot, lo, hi):
        for base, count, fetch in self.phases:
            if base + count <= lo or hi < base:
                continue
            if lo == hi or (base <= lo and hi < base + count):
                fetch(t - base, self.wbuf.at[slot], self.wsem.at[slot])
            else:
                @pl.when((t >= base) & (t < base + count))
                def _(base=base, fetch=fetch):
                    fetch(t - base, self.wbuf.at[slot], self.wsem.at[slot])

    def prologue(self):
        for t in range(min(self.depth, self.total)):
            self.issue(t, t, t, t)

    def run(self, phase, group, body):
        base, count, _ = self.phases[phase]

        @pl.loop(0, count // group)
        def _(i):
            first = i * group + base
            slots = [(first + k) % self.depth for k in range(group)]
            for slot in slots:
                local(self.like, self.wbuf.at[slot], self.wsem.at[slot]).wait()
            body(i, [self.wbuf.at[slot] for slot in slots])
            for k, slot in enumerate(slots):
                self.issue(first + k + self.depth, slot, base + self.depth, base + count - 1 + self.depth)


def col_tiles(w_ref, layer, g, width, row_chunks):
    def issue(i, buf, sem):
        ci, ri = i // row_chunks, i % row_chunks
        at = pl.ds(pl.multiple_of(g * width + ci * TC, TC), TC)
        src = w_ref.at[span(ri, TR), at] if layer < 0 else w_ref.at[layer, span(ri, TR), at]
        local(src, buf, sem).start()
    return issue


def kv_tiles(wk_ref, wv_ref, layer, g):
    def issue(i, buf, sem):
        for k, w_ref in enumerate((wk_ref, wv_ref)):
            local(w_ref.at[layer, span(i, TR), span(g, KW)], buf.at[:, pl.ds(k * KW, KW)], sem).start()
    return issue


def gate_up_tiles(wg_ref, wu_ref, layer, g):
    def issue(i, buf, sem):
        at = pl.ds(pl.multiple_of(g * FW + (i // G) * TC, TC), TC)
        for k, w_ref in enumerate((wg_ref, wu_ref)):
            @pl.when((i // HT) % 2 == k)
            def _():
                local(w_ref.at[layer, span(i % HT, TR), at], buf, sem).start()
    return issue


def norm_into(r_ref, g_row, hbuf):
    total = rsum(r_ref[0] * r_ref[0])
    for k in range(1, G):
        total = total + rsum(r_ref[k] * r_ref[k])
    inv = lax.rsqrt(total / D + NORM_EPS)
    for k in range(G):
        gain = g_row[:, cols(k, QW)].astype(F32)
        hbuf[k // 2, :, cols(k % 2, QW)] = (r_ref[k] * inv * gain).astype(BF16)


def rope(x_bf, cos_row, sin_row):
    v = x_bf.astype(F32)
    return (v * cos_row + pltpu.roll(v, HALF, 1) * sin_row).astype(BF16)


def stream_q(stream, part, hbuf, acc, cos_row, sin_row, out_ref, first=0):
    def body(i, w):
        acc[i + HT * part] = mm(hbuf[0], w[0][:]) + mm(hbuf[1], w[1][:])

    stream.run(first + part, HT, body)
    for head in (range(KVH), range(KVH, QKV // HD))[part]:
        piece = acc[head // G, :, cols(head % G, HD)].astype(BF16)
        if head * HD < QW + KW:
            piece = rope(piece, cos_row, sin_row)
        out_ref[:, cols(head, HD)] = piece


def my_half(piece, c):
    wide = piece.astype(F32)
    return jnp.where(c == 0, wide[:NB], wide[NB:])


def spread_kv(buf, base, c, out_ref, at):
    for k in range(G):
        for j in range(G):
            part, h = j // 2, j % 2
            out_ref[:, at + part * KVH + 2 * k + h, :] = my_half(buf[base + k, :, QW + j * HD:QW + (j + 1) * HD], c)


def own_start(buf, g, sems, k0, peers, x):
    return start_all([remote(buf.at[g], buf.at[g], sems.at[0, k0, k], sems.at[1, k0, k], peer(x, *p))
                      for k, p in enumerate(peers)])


def kernel_table(par_ref, meta_ref, choice_ref, bucket_ref):
    square = (NA, NA)
    i, j = iota(square, 0), iota(square, 1)
    par_row = jnp.broadcast_to(par_ref[:], square)
    par_col = rsum(jnp.where(i == j, par_row, 0).astype(F32)).astype(I32)
    fi, fj = i.astype(F32), j.astype(F32)

    def flag(v):
        return jnp.where(v, 1.0, 0.0)

    same, same_t = par_col == j, par_row == i
    far, half = (i // NX) != (j // NX), (i // NX) == (j // NX)
    before = rsum(flag((par_row < par_col) | ((par_row == par_col) & (j < i))))
    cross_row = jnp.minimum(csum(flag(same & far)), 1.0)
    cross_col = jnp.minimum(rsum(flag(same_t & far)), 1.0)
    place_col = rsum(flag(half & (j < i)) * cross_row)
    slot_col = place_col + (i // NX * NX).astype(F32)[:, :1]
    code = jnp.where(par_row // NB == j // NB, 0.0, jnp.where(par_row // NX == j // NX, 1.0, 2.0))[:1]
    place_par = csum(flag(same_t) * place_col)
    lane = j[:1]
    used = [rsum(jnp.where(lane // NX == k, cross_row, 0.0)) for k in range(2)]
    extra = jnp.maximum(used[0], used[1]) - (ONE + FIX)
    most = extra + FIX
    bucket = flag(extra > BUCKETS[0])
    choice = flag(most > FIXES[0]) + flag(most > FIXES[1])
    choice_ref[0] = choice.astype(I32)[0, 0]
    for n in BUCKETS[1:]:
        bucket = bucket + flag(extra > n)
    bucket_ref[0] = bucket.astype(I32)[0, 0]
    misc = jnp.where(lane == 0, used[0], used[1])
    rows = [csum(jnp.where(before == fj, fi, 0.0)), csum(flag(par_col < j)), csum(flag(same)),
            csum(jnp.where(slot_col == fj, fi, 0.0) * cross_col), code,
            jnp.where(code > 1.0, place_par, (par_row % NB).astype(F32)[:1]), misc, par_row[:1].astype(F32)]
    for k, row in enumerate(rows):
        meta_ref[k:k + 1, :NA] = row.astype(I32)


def kernel_a(tok_ref, score_ref, cos_ref, sin_ref, ga_ref, wq_ref, wk_ref, wv_ref, k_ref, v_ref,
             q_out, kv_out, own_out, r_out, score_out, xp1_out, xp0_out,
             wbuf, wsem, tokx, scx, r_s, hbuf, acc, qkvx, ssem, rsem, xsem):
    x, y, c = coords()
    g = y * 2 + c
    d = x * G + g
    stream = Stream(wbuf, wsem, [(G, col_tiles(wq_ref, 0, g, QW, HT)), (HT, kv_tiles(wk_ref, wv_ref, 0, g))],
                    wq_ref.at[0, pl.ds(0, TR), pl.ds(0, TC)])
    stream.prologue()
    others = all_peers(x, y, c)
    barrier_with([peer(*p) for p in others])
    tok_copy = remote(tok_ref, tokx, ssem.at[0], rsem.at[0], peer(x, y, 1 - c))
    tok_copy.start()
    beam = 2 * x + c
    for i in range(NB):
        scx[beam, i:i + 1, :] = jnp.full((1, HD), score_ref[i], F32)
    for k in range(G):
        r_s[k, span(c, NB), :] = tok_ref[:, cols(k, QW)].astype(F32)
    sc_copies = start_all([remote(scx.at[beam], scx.at[beam], ssem.at[k], rsem.at[k], peer(xx, y, cc))
                           for k, (xx, cc) in enumerate(((1 - x, c), (1 - x, 1 - c), (x, 1 - c)), 1)])
    beside = peer(x, y, 1 - c)
    send_part(k_ref, v_ref, 1, 1 - c, xp1_out, xsem.at[0], beside)
    send_part(k_ref, v_ref, 0, 1 - c, xp0_out, xsem.at[1], beside)
    tok_copy.wait()
    for k in range(G):
        r_s[k, span(1 - c, NB), :] = tokx[:, cols(k, QW)].astype(F32)
    norm_into(r_s, ga_ref[0:1, :], hbuf)
    for i in range(HT):
        stream_q(stream, i, hbuf, acc, cos_ref[:], sin_ref[:], qkvx.at[d])
        own = qkvx.at[d]
        piece = own.at[:, pl.ds(0, QW)] if i == 0 else own.at[:, pl.ds(QW, 2 * KW)]
        copies = start_all([remote(piece, piece, ssem.at[G * (i + 1) + k], rsem.at[G * (i + 1) + k], peer(*p))
                            for k, p in enumerate(others) if i == 0 or k >= G])
        if i == 0:
            q_copies = copies
    own_out[:] = qkvx[d]
    r_out[:] = r_s[:]
    wait_all(sc_copies)
    for k in range(G):
        score_out[cols(k, NB), :] = scx[k]

    def spread_q(dd):
        for h in range(KVH):
            q_out[span(dd // G, NX), dd % G * KVH + h, :] = qkvx[dd, :, cols(h, HD)].astype(F32)

    spread_q(d)
    wait_all(copies)
    spread_kv(qkvx, x * G, c, kv_out, 0)
    for k in range(len(others) - 1, -1, -1):
        q_copies[k].wait()
        xx, yy, cc = others[k]
        spread_q(xx * G + yy * 2 + cc)
    wait_part(xp1_out, xsem.at[0], beside)
    wait_part(xp0_out, xsem.at[1], beside)


def send_rows(ref, layer, half, out, send_sem, recv_sem, dev):
    @pl.loop(0, NB // 2)
    def _(r):
        at = half * (NB // 2) + r
        remote(ref.at[layer, at], out.at[at], send_sem, recv_sem, dev).start()


def send_part(k_ref, v_ref, layer, part, out, xsem, dev):
    for k, ref in enumerate((k_ref, v_ref)):
        @pl.when(part == k)
        def _():
            @pl.loop(0, NB)
            def _(r):
                remote(ref.at[layer, r], out.at[r], xsem.at[0], xsem.at[1], dev).start()


def wait_part(out, xsem, dev):
    remote(out, out, xsem.at[0], xsem.at[1], dev).wait()


def mask_bias(limit):
    row, col = iota((NA, ROWS), 0), iota((NA, ROWS), 1)
    ok = ((col % KVH) == (row // G)) & (col < limit * KVH)
    return jnp.where(ok, 0.0, NEG)


def attend(q, k_rows, v_rows, bias):
    s = lax.dot_general(q, k_rows, (((1,), (1,)), ((), ())), preferred_element_type=F32)
    s = (s.reshape(-1, NA, ROWS) + bias[:]).reshape(s.shape)
    m = rmax(s)
    e = jnp.exp2((s - m) * EXP2)
    return mm(e.astype(BF16), v_rows), m * SCALE, rsum(e)


def to_lanes(column):
    return csum(jnp.where(iota((NA, HD), 0) == iota((NA, HD), 1), column, 0.0))


def keep(o_ref, st_ref, b, o, m, total):
    o_ref[b] = o
    st_ref[0, pl.ds(b, 1), :] = to_lanes(m)
    st_ref[1, pl.ds(b, 1), :] = to_lanes(total)


def kernel_home(meta, pos_ref, q_ref, k_ref, v_ref, o_ref, st_ref, kbuf, vbuf, bias, ksem, vsem):
    x, y, c = coords()
    first = (2 * x + c) * NB
    limit = jnp.clip(pos_ref[0] - y * SLOTS, 0, SLOTS)

    def count_of(r):
        return jnp.where(limit > 0, meta[T_COUNT, first + r], 0)

    def copies(r):
        return local(k_ref.at[0, r], kbuf.at[r], ksem.at[r]), local(v_ref.at[0, r], vbuf.at[r], vsem.at[r])

    @pl.loop(0, NB)
    def _(r):
        @pl.when(count_of(r) > 0)
        def _():
            start_all(copies(r))

    o_ref[:] = jnp.zeros_like(o_ref)
    st_ref[0] = jnp.full((NA, HD), NEG, F32)
    st_ref[1] = jnp.zeros((NA, HD), F32)
    bias[:] = mask_bias(limit)

    @pl.loop(0, NB)
    def _(r):
        count = count_of(r)
        start = meta[T_START, first + r]

        @pl.when(count > 0)
        def _():
            wait_all(copies(r))

        def step(s, carry):
            beams = [meta[T_ORDER, start + jnp.minimum(s * G + j, count - 1)] for j in range(G)]
            q = jnp.concatenate([q_ref[b] for b in beams], axis=0).astype(BF16)
            o, m, total = attend(q, kbuf[r], vbuf[r], bias)
            for j, b in enumerate(beams):
                at = cols(j, NA)
                keep(o_ref, st_ref, b, o[at], m[at], total[at])
            return carry

        lax.fori_loop(0, (count + G - 1) // G, step, 0)


def lane_pick(rows, lane):
    return rsum(jnp.where(iota(rows.shape, 1) == lane, rows, 0.0))


def send_partials(o_ref, st_ref, ox, sx, x, g, d, others, psem):
    copies = []
    for k, (xx, yy, cc) in enumerate(others):
        beams, heads, dev = span(xx, NX), span(yy * 2 + cc, KVH), peer(xx, yy, cc)
        copies.append(remote(st_ref.at[:, beams, :], sx.at[d], psem.at[0, 0, k], psem.at[1, 0, k], dev))
        copies.append(remote(o_ref.at[beams, heads, :], ox.at[d], psem.at[0, 1, k], psem.at[1, 1, k], dev))
    start_all(copies)
    sx[d] = st_ref[:, span(x, NX), :]
    ox[d] = o_ref[span(x, NX), span(g, KVH), :]
    return copies


def combine_first(copies, own_ref, ox, sx, g, out_ref):
    lanes = iota((NX, HD), 1)
    s_self = jnp.full((NX, HD), NEG, F32)
    for h in range(KVH):
        q = own_ref[:, cols(h, HD)].astype(F32)
        kk = own_ref[:, cols(KVH + h // G, HD)].astype(F32)
        s_self = jnp.where(lanes == g * KVH + h, rsum(q * kk) * SCALE, s_self)
    wait_all(copies)
    top = s_self
    for i in range(2 * G):
        top = jnp.maximum(top, sx[i, 0])
    e_self = jnp.exp(s_self - top)
    total = e_self
    weights = []
    for i in range(2 * G):
        weights.append(jnp.exp(sx[i, 0] - top))
        total = total + weights[i] * sx[i, 1]
    for h in range(KVH):
        lane = g * KVH + h
        vv = own_ref[:, cols(KVH + 2 + h // G, HD)].astype(F32)
        mix = lane_pick(e_self, lane).astype(BF16).astype(F32) * vv
        for i in range(2 * G):
            mix = mix + lane_pick(weights[i], lane) * ox[i, :, h, :]
        out_ref[:, cols(h, HD)] = (mix / lane_pick(total, lane)).astype(BF16)


class Crossing:
    def __init__(self, x, y, c, rows, sems):
        self.first, self.second = [], []
        for k, (src, got, passed) in enumerate(rows):
            if src is not got:
                self.first.append(remote(src, got, sems.at[0, k], sems.at[1, k], peer(1 - x, y, c)))
            self.second.append(remote(got, passed, sems.at[2, k], sems.at[3, k], peer(x, y, 1 - c)))
        self.ready = len(self.second) - len(self.first)

    def start(self):
        start_all(self.first)
        start_all(self.second[:self.ready])

    def forward(self, k):
        self.first[k].wait_recv()
        self.second[self.ready + k].start()

    def finish(self, k):
        for i in range(k, len(self.first)):
            self.forward(i)
        for cp in self.first:
            cp.wait_send()
        wait_all(self.second)


def one_and_fix(n, one_ref, one_p, fix_ref, fix_r, fix_p):
    here = one_ref.at[0]
    return [(here, here, one_p.at[0])] + [(fix_ref.at[k], fix_r.at[k], fix_p.at[k]) for k in range(n)]


def out_mlp(stream, first, g, x, peers, r_s, hbuf, acc, ox, yx, zx, ubuf, gm_row, sems, usem, cross, side):
    def half_sends(buf, k0, i):
        buf[g, i] = acc[i].astype(BF16)
        start_all([remote(buf.at[g, i], buf.at[g, i], sems.at[0, k0, k], sems.at[1, k0, k], peer(x, *p))
                   for k, p in enumerate(peers)])

    def add(buf, k0):
        wait_all([remote(buf.at[g], buf.at[g], sems.at[0, k0, k], sems.at[1, k0, k], peer(x, *p)) for k, p in enumerate(peers)])
        for k in range(G):
            for i in range(HT):
                r_s[k, :, cols(i, TC)] = r_s[k, :, cols(i, TC)] + buf[k, i].astype(F32)

    copies = own_start(ox, g, sems, 0, peers, x)
    wait_all(copies)
    for k in range(G):
        hbuf[k // 2, :, cols(k % 2, QW)] = ox[k]

    def project(w):
        return mm(hbuf[0], w[0][:]) + mm(hbuf[1], w[1][:])

    def body_out(i, w):
        acc[i] = project(w)
        half_sends(yx, 1, i)

    stream.run(first, HT, body_out)
    add(yx, 1)
    norm_into(r_s, gm_row, hbuf)

    def body_gu(i, w):
        side(i)
        gate = project(w[:HT]).astype(BF16).astype(F32)
        up = project(w[HT:]).astype(BF16).astype(F32)
        at = g * UT + i
        ubuf[at] = (jax.nn.silu(gate) * up).astype(BF16)
        start_all([remote(ubuf.at[at], ubuf.at[at], usem.at[0, k], usem.at[1, k], peer(x, *p))
                   for k, p in enumerate(peers)])

    stream.run(first + 1, G, body_gu)
    cross.forward(0)
    mine = ubuf.at[pl.ds(g * UT, UT)]
    wait_all([remote(mine, mine, usem.at[0, k], usem.at[1, k], peer(x, *p)) for k, p in enumerate(peers)])

    def body_down(i, w):
        total = mm(ubuf[0], w[0][cols(0, TC), :])
        for k in range(1, UC):
            total = total + mm(ubuf[k], w[k // G][cols(k % G, TC), :])
        acc[i] = total
        half_sends(zx, 2, i)

    stream.run(first + 2, UT, body_down)
    add(zx, 2)


def mlp_phases(layer, g, wo_ref, wg_ref, wu_ref, wd_ref):
    return [(G, col_tiles(wo_ref, layer, g, QW, HT)),
            (UC, gate_up_tiles(wg_ref, wu_ref, layer, g)),
            (2 * UT, col_tiles(wd_ref, layer, g, QW, UT))]


def kernel_mid(n, o_ref, st_ref, own_ref, r_ref, cos_ref, sin_ref, ga_ref, gm_ref, wo_ref, wg_ref, wu_ref, wd_ref, wq_ref, wk_ref, wv_ref,
               k_ref, v_ref, one_ref, fix_ref,
               qkv_out, r_out, one_p, fix_r, fix_p, xq1_out, xq0_out,
               wbuf, wsem, r_s, hbuf, acc, ox, yx, zx, ubuf, qkvx, px, sx, sems, usem, csem, xsem, psem):
    x, y, c = coords()
    g = y * 2 + c
    peers = group_peers(x, y, c)
    stream = Stream(wbuf, wsem, mlp_phases(0, g, wo_ref, wg_ref, wu_ref, wd_ref) + [
        (G, col_tiles(wq_ref, 1, g, QW, HT)), (HT, kv_tiles(wk_ref, wv_ref, 1, g))],
        wq_ref.at[0, pl.ds(0, TR), pl.ds(0, TC)])
    stream.prologue()
    beside = peer(x, y, 1 - c)
    others = all_peers(x, y, c)
    barrier_with([peer(*p) for p in others])
    cross = Crossing(x, y, c, one_and_fix(n, one_ref, one_p, fix_ref, fix_r, fix_p), csem)
    partials = send_partials(o_ref, st_ref, px, sx, x, g, x * G + g, others, psem)
    cross.start()
    r_s[:] = r_ref[:]
    combine_first(partials, own_ref, px, sx, g, ox.at[g])

    def side(i):
        for layer, out in ((1, xq1_out), (0, xq0_out)):
            for k, ref in enumerate((k_ref, v_ref)):
                @pl.when((i // 2 == 1 - layer) & (c == k))
                def _():
                    send_rows(ref, layer, i % 2, out, xsem.at[0, layer], xsem.at[1, layer], beside)

    out_mlp(stream, 0, g, x, peers, r_s, hbuf, acc, ox, yx, zx, ubuf, gm_ref[0:1, :], sems, usem, cross, side)
    cross.forward(1)
    norm_into(r_s, ga_ref[1:2, :], hbuf)
    for i in range(HT):
        stream_q(stream, i, hbuf, acc, cos_ref[:], sin_ref[:], qkvx.at[g], 3)
        own = qkvx.at[g]
        piece = own.at[:, pl.ds(0, QW)] if i == 0 else own.at[:, pl.ds(QW, 2 * KW)]
        copies = start_all([remote(piece, piece, sems.at[0, 3 * i, k], sems.at[1, 3 * i, k], peer(x, *p)) for k, p in enumerate(peers)])
        if i == 0:
            q_copies = copies
    cross.forward(2)
    r_out[:] = r_s[:]
    for k, out in enumerate((xq0_out, xq1_out)):
        remote(out, out, xsem.at[0, k], xsem.at[1, k], beside).wait()
    wait_all(q_copies + copies)
    for k in range(G):
        for h in range(KVH):
            qkv_out[:, k * KVH + h, :] = my_half(qkvx[k, :, cols(h, HD)], c)
    spread_kv(qkvx, 0, c, qkv_out, NA)
    cross.finish(3)


def kernel_end(n, o_ref, st_ref, r_ref, gm_ref, gf_ref, wo_ref, wg_ref, wu_ref, wd_ref, wvoc_ref,
               one_ref, fix_ref,
               candx, log_out, one_p, fix_r, fix_p,
               wbuf, wsem, r_s, hbuf, acc, ox, yx, zx, ubuf, px, sx, lbuf, stx, run_st,
               sems, usem, psem, lsem, csem):
    x, y, c = coords()
    g = y * 2 + c
    peers = group_peers(x, y, c)
    stream = Stream(wbuf, wsem, mlp_phases(1, g, wo_ref, wg_ref, wu_ref, wd_ref) + [
        (VW // TC * HT, col_tiles(wvoc_ref, -1, g, VW, HT))],
        wvoc_ref.at[pl.ds(0, TR), pl.ds(0, TC)])
    stream.prologue()
    barrier_with([peer(x, *p) for p in peers] + [peer(1 - x, y, c)])
    cross = Crossing(x, y, c, one_and_fix(n, one_ref, one_p, fix_ref, fix_r, fix_p), csem)
    cross.start()
    copies = []
    for k, (yy, cc) in enumerate(peers):
        heads, dev = span(yy * 2 + cc, KVH), peer(x, yy, cc)
        copies.append(remote(st_ref, sx.at[g], psem.at[0, 0, k], psem.at[1, 0, k], dev))
        copies.append(remote(o_ref.at[:, heads, :], px.at[g], psem.at[0, 1, k], psem.at[1, 1, k], dev))
    start_all(copies)
    sx[g] = st_ref[:]
    px[g] = o_ref[:, span(g, KVH), :]
    r_s[:] = r_ref[:]
    wait_all(copies)
    for cc in range(2):
        pair = (cc, 2 + cc)
        top = jnp.maximum(sx[pair[0], 0], sx[pair[1], 0])
        weights = [jnp.exp(sx[p, 0] - top) for p in pair]
        total = weights[0] * sx[pair[0], 1] + weights[1] * sx[pair[1], 1]
        for h in range(KVH):
            lane = g * KVH + h
            mix = lane_pick(weights[0], lane) * px[pair[0], :, h, :] + lane_pick(weights[1], lane) * px[pair[1], :, h, :]
            acc[h // G, cols(cc, NB), cols(h % G, HD)] = mix / lane_pick(total, lane)
    for k in range(HT):
        ox[g, :, cols(k, TC)] = acc[k].astype(BF16)
    out_mlp(stream, 0, g, x, peers, r_s, hbuf, acc, ox, yx, zx, ubuf, gm_ref[1:2, :], sems, usem, cross, lambda i: i)
    cross.forward(1)
    norm_into(r_s, gf_ref[:], hbuf)
    run_st[0] = jnp.full((NX, HD), NEG, F32)
    run_st[1] = jnp.zeros((NX, HD), F32)
    nv = VW // TC

    def body_voc(i, w):
        logits = mm(hbuf[0], w[0][:]) + mm(hbuf[1], w[1][:])
        for cc in range(2):
            lbuf[i, cc] = logits[cols(cc, NB)]
        at = g * nv + i
        candx[at] = lbuf[i, c]
        start_all([remote(lbuf.at[i, cc], candx.at[at], lsem.at[0, k], lsem.at[1, k], peer(x, yy, cc))
                   for k, (yy, cc) in enumerate(peers)])
        old = run_st[0][:, :1]
        top = jnp.maximum(old, rmax(logits))
        run_st[1] = run_st[1] * jnp.exp(old - top) + rsum(jnp.exp(logits - top))
        run_st[0] = jnp.broadcast_to(top, (NX, HD))

    stream.run(3, HT, body_voc)
    stx[g] = run_st[:]
    wait_all(own_start(stx, g, sems, 3, peers, x))
    tops = [stx[k, 0, span(c, NB), :] for k in range(G)]
    top = functools.reduce(jnp.maximum, tops)
    total = sum(stx[k, 1, span(c, NB), :] * jnp.exp(tops[k] - top) for k in range(G))
    log_out[:] = top + jnp.log(total)
    got = candx.at[pl.ds(g * nv, nv)]
    wait_all([remote(lbuf.at[:, cc], got, lsem.at[0, k], lsem.at[1, k], peer(x, yy, cc)) for k, (yy, cc) in enumerate(peers)])
    cross.finish(2)


def kernel_pack(layer, meta, dep, k_ref, v_ref, xp_ref, one, fix, rest, buf, isem, osem):
    x, y, c = coords()
    count = meta[T_MISC, x]
    segments = ((one, 0, ONE), (fix, ONE, ONE + FIX), (rest, ONE + FIX, NX))

    def fetch(p):
        v = meta[T_LIST, x * NX + p]
        r, own = v % NB, (v // NB) % 2 == c
        for core, mine in enumerate((k_ref, v_ref)):
            @pl.when((c == core) & own)
            def _():
                local(mine.at[layer, r], buf.at[p], isem.at[p]).start()

        @pl.when(jnp.logical_not(own))
        def _():
            local(xp_ref.at[r], buf.at[p], isem.at[p]).start()

    def store(p, op):
        for ref, lo, hi in segments:
            @pl.when((p >= lo) & (p < hi))
            def _():
                op(local(buf.at[p], ref.at[jnp.clip(p - lo, 0, hi - lo - 1)], osem.at[p]))

    def each(fn):
        lax.fori_loop(0, count, lambda p, z: (fn(p), z)[1], 0)

    def move(p):
        local(xp_ref.at[0], buf.at[p], isem.at[p]).wait()
        store(p, lambda cp: cp.start())

    each(fetch)
    each(move)
    each(lambda p: store(p, lambda cp: cp.wait()))


def fetch_row(layer, meta, b, mine, own_ref, partner, crossed, dst, sem):
    code, idx = meta[T_CODE, b], meta[T_IDX, b]

    @pl.when(code == 0)
    def _():
        local(own_ref.at[layer, idx % NB], dst, sem).start()

    for ref, cond in zip(partner, (mine, jnp.logical_not(mine))):
        @pl.when((code == 1) & cond)
        def _():
            local(ref.at[idx % NB], dst, sem).start()

    for lo, hi, refs in crossed:
        for ref, cond in zip(refs, (mine, jnp.logical_not(mine))):
            @pl.when((code == 2) & (idx >= lo) & (idx < hi) & cond)
            def _():
                local(ref.at[jnp.clip(idx - lo, 0, hi - lo - 1)], dst, sem).start()


def put_new(buf, i, new, at):
    rows = span(at // 2, NX)
    hit = iota((NX, HD), 0) // KVH == at % 2
    both = jnp.concatenate([new, new], axis=0)
    buf[i, rows, :] = jnp.where(hit, both, buf[i, rows, :].astype(F32)).astype(BF16)


def kernel_child(layer, *refs):
    if layer:
        (meta, pos_ref, new_ref, score_ref, k_ref, v_ref, xp, xq, *moved,
         ko, vo, o_ref, st_ref, score_out, kbuf, vbuf, isem, osem, bias) = refs
        at0 = NA
    else:
        (meta, pos_ref, new_ref, score_ref, logits_ref, log_ref, k_ref, v_ref, xp, xq, *moved, _, _,
         ko, vo, cand_ref, kbuf, vbuf, isem, osem, logit_buf, cand_buf, csem) = refs
        at0 = 0
        logits_in = local(logits_ref, logit_buf, csem.at[0])
        logits_in.start()
    x, y, c = coords()
    first = (2 * x + c) * NB
    pos = pos_ref[0] - y * SLOTS
    one_r, one_p, fix_r, fix_p, rest_r, rest_p = moved
    crossed = ((0, ONE, (one_r, one_p)), (ONE, ONE + FIX, (fix_r, fix_p)), (ONE + FIX, NX, (rest_r, rest_p)))
    both = ((k_ref, kbuf, ko), (v_ref, vbuf, vo))

    @pl.loop(0, NB)
    def _(i):
        for part, (src, buf, _) in enumerate(both):
            fetch_row(layer, meta, first + i, c == part, src, (xp, xq), crossed, buf.at[i], isem.at[part, i])

    if layer:
        bias[:] = mask_bias(jnp.clip(pos + 1, 1, SLOTS))
    else:
        logits_in.wait()

        @pl.loop(0, G * VW // TC, unroll=G)
        def _(i):
            cand_buf[:, span(i, TC)] = score_ref[:, :1] + (logit_buf[i] - log_ref[:, :1])

        cand_copy = local(cand_buf, cand_ref, csem.at[1])
        cand_copy.start()

    @pl.loop(0, NB)
    def _(i):
        for part, (src, buf, out) in enumerate(both):
            local(src.at[0, 0], buf.at[i], isem.at[part, i]).wait()

            @pl.when((pos >= 0) & (pos < SLOTS))
            def _():
                start = at0 + part * KVH
                put_new(buf, i, new_ref[i, start:start + KVH, :], jnp.clip(pos, 0, SLOTS - 1))

            local(buf.at[i], out.at[layer, i], osem.at[part, i]).start()
        if layer:
            keep(o_ref, st_ref, i, *attend(new_ref[i, :NA, :].astype(BF16), kbuf[i], vbuf[i], bias))
            score_out[pl.ds(i, 1), :] = score_ref[pl.ds(meta[T_PAR, first + i], 1), :]

    @pl.loop(0, NB)
    def _(i):
        for part, (_, buf, out) in enumerate(both):
            local(buf.at[i], out.at[layer, i], osem.at[part, i]).wait()

    if not layer:
        cand_copy.wait()


def kernel_rest(n, src, got, passed, sems):
    x, y, c = coords()
    barrier_with([peer(1 - x, y, c), peer(x, y, 1 - c)])
    cross = Crossing(x, y, c, [(src.at[i], got.at[i], passed.at[i]) for i in range(n)], sems)
    cross.start()
    cross.finish(0)


def shape(s, t=BF16):
    return jax.ShapeDtypeStruct(s, t)


def rows_of(n):
    return shape((n,) + ROW)


def scratch_stream(n=MANY):
    return [pltpu.VMEM((n, TR, TC), BF16), DMA((n,))]


def scratch_mlp():
    wide = (G, NX, QW)
    return [pltpu.VMEM(wide, F32), pltpu.VMEM((HT, NX, TR), BF16), pltpu.VMEM((HT + 1, NX, TC), F32),
            pltpu.VMEM(wide, BF16), pltpu.VMEM((G, HT, NX, TC), BF16), pltpu.VMEM((G, HT, NX, TC), BF16),
            pltpu.VMEM((UC, NX, TC), BF16)]


def call(kernel, name, us, outs, ins, scratch, cid=-1, aliases=()):
    more = {} if cid < 0 else dict(collective_id=cid, has_side_effects=True)
    return pl.pallas_call(
        kernel, out_shape=tuple(o for o, _ in outs), in_specs=ins, out_specs=tuple(s for _, s in outs),
        scratch_shapes=scratch, input_output_aliases=dict(aliases), name=name,
        cost_estimate=pl.CostEstimate(flops=us * 400000000, bytes_accessed=us * 3000000, transcendentals=0),
        compiler_params=pltpu.CompilerParams(vmem_limit_bytes=59 * 2 ** 20, **more))


def solution(mesh):
    beam_spec = P(('dp', 'beam'))
    row_spec = P(('dp', 'beam'), None)
    cache_spec = P(None, ('dp', 'beam'), 'sp', None, None)
    full_rep = P()
    swap_x = [(b, (b + 2) % G) for b in range(G)]

    def rest(index, packed):
        def branch(k, n):
            outs = [(rows_of(REST), HB)] * 2
            if n == 0:
                return call(lambda *_: None, 'rest_none', 1, outs, [HB], [])
            return call(functools.partial(kernel_rest, n), f'rest_{n}', 1, outs, [HB], [DMA((4, n))], NX + k)
        return lax.switch(index, [branch(k, n) for k, n in enumerate(BUCKETS)], packed)

    def local_step(tok_emb, parent, position, beam_score, k_cache, v_cache, w_query, w_key, w_value, w_out, w_gate, w_up, w_down, g_attn, g_mlp, g_final, w_vocab):
        cur_pos = position[0]
        half = jnp.arange(HD, dtype=I32) % HALF
        inv_freq = ROPE_BASE ** (-2.0 * half.astype(F32) / HD)
        angles = (cur_pos.astype(F32) * inv_freq)[None, :]
        cos_row = jnp.cos(angles)
        sin_row = jnp.sin(angles) * jnp.where(jnp.arange(HD) < HALF, -1.0, 1.0)
        kc, vc = k_cache.reshape((2, NB) + ROW), v_cache.reshape((2, NB) + ROW)
        lanes = shape((NA, HD), F32)
        logits = shape((G * VW // TC, NB, TC), F32)

        meta, choice, bucket = call(kernel_table, 'table', 2, [(shape((NB, HD), I32), VM), (shape((1,), I32), SM), (shape((1,), I32), SM)], [VM], [])(parent)
        choice, bucket = choice.reshape(()), bucket.reshape(())

        def chosen(kernel, name, us, outs, ins, scratch, cid):
            return lambda *args: lax.switch(choice, [
                call(functools.partial(kernel, n), f'{name}_{n}', us, outs, ins, scratch, cid + n) for n in FIXES], *args)

        q0, kv0, own0, r0, scores, xp1, xp0 = call(
            kernel_a, 'qkv_first', 12,
            [(shape((NA, NA, HD), F32), VM), (shape((NB, NX, HD), F32), VM), (shape((NX, QKV)), VM),
             (shape((G, NX, QW), F32), VM), (lanes, VM), (rows_of(NB), HB), (rows_of(NB), HB)],
            [VM, SM, VM, VM, VM] + [HB] * 5,
            scratch_stream(FEW) + [
                pltpu.VMEM((NB, D), BF16), pltpu.VMEM((G, NB, HD), F32), pltpu.VMEM((G, NX, QW), F32),
                pltpu.VMEM((HT, NX, TR), BF16), pltpu.VMEM((HT + 1, NX, TC), F32), pltpu.VMEM((2 * G, NX, QKV), BF16),
                DMA((G * G,)), DMA((G * G,)), DMA((2, 2))], 1,
        )(tok_emb, beam_score, cos_row, sin_row, g_attn, w_query, w_key, w_value, kc, vc)

        def pack_rows(layer, dep, xp):
            return call(functools.partial(kernel_pack, layer), f'pack_{layer}', 3,
                        [(rows_of(ONE), HB), (rows_of(FIX), HB), (rows_of(REST), HB)], [SM] + [HB] * 4,
                        [pltpu.VMEM((NX,) + ROW, BF16), DMA((NX,)), DMA((NX,))])(meta, dep, kc, vc, xp)

        one1, fix1, rest1 = pack_rows(1, own0, xp1)
        one_r1 = lax.ppermute(one1, 'beam', swap_x)
        o0, st0 = call(
            kernel_home, 'attend_home', 9, [(shape((NA, NA, HD), F32), VM), (shape((2, NA, HD), F32), VM)],
            [SM, SM, VM, HB, HB],
            [pltpu.VMEM((NB,) + ROW, BF16)] * 2 + [pltpu.VMEM((NA, ROWS), F32), DMA((NB,)), DMA((NB,))],
        )(meta, position, q0, kc, vc)

        one0, fix0, rest0 = pack_rows(0, st0, xp0)

        weights = (w_out, w_gate, w_up, w_down)
        qkv1, r1, one_p1, fix_r1, fix_p1, xq1, xq0 = chosen(
            kernel_mid, 'mlp_first', 50,
            [(shape((NB, NA + NX, HD), F32), VM), (shape((G, NX, QW), F32), VM), (rows_of(ONE), HB),
             (rows_of(FIX), HB), (rows_of(FIX), HB), (rows_of(NB), HB), (rows_of(NB), HB)],
            [VM] * 8 + [HB] * 11,
            scratch_stream() + scratch_mlp() + [
                pltpu.VMEM((G, NX, QKV), BF16), pltpu.VMEM((2 * G, NX, KVH, HD), F32), pltpu.VMEM((2 * G, 2, NX, HD), F32),
                DMA((2, G, 3)), DMA((2, 3)), DMA((4, ONE + FIX)), DMA((2, 2)), DMA((2, 2, 7))], 0,
        )(o0, st0, own0, r0, cos_row, sin_row, g_attn, g_mlp, *weights, w_query, w_key, w_value, kc, vc, one_r1, fix1)

        rest1, _ = lax.optimization_barrier((rest1, r1))
        rest_r1, rest_p1 = rest(bucket, rest1)

        one0, _ = lax.optimization_barrier((one0, rest_r1))
        one_r0 = lax.ppermute(one0, 'beam', swap_x)
        child_scratch = [pltpu.VMEM((NB,) + ROW, BF16), pltpu.VMEM((NB,) + ROW, BF16), DMA((2, NB)), DMA((2, NB))]
        cache_out = [(shape((2, NB) + ROW), HB)] * 2
        ko, vo, o1, st1, score1 = call(
            functools.partial(kernel_child, 1), 'attend_child', 9,
            cache_out + [(shape((NB, NA, HD), F32), VM), (shape((2, NB, HD), F32), VM), (shape((NB, HD), F32), VM)],
            [SM, SM, VM, VM] + [HB] * 10, child_scratch + [pltpu.VMEM((NA, ROWS), F32)],
        )(meta, position, qkv1, scores, kc, vc, xp1, xq1, one_r1, one_p1, fix_r1, fix_p1, rest_r1, rest_p1)

        logit, log_z, one_p0, fix_r0, fix_p0 = chosen(
            kernel_end, 'mlp_vocab', 58,
            [(logits, VM), (shape((NB, HD), F32), VM), (rows_of(ONE), HB), (rows_of(FIX), HB), (rows_of(FIX), HB)],
            [VM] * 5 + [HB] * 7,
            scratch_stream() + scratch_mlp() + [
                pltpu.VMEM((G, NB, KVH, HD), F32), pltpu.VMEM((G, 2, NB, HD), F32),
                pltpu.VMEM((VW // TC, 2, NB, TC), F32), pltpu.VMEM((G, 2, NX, HD), F32),
                pltpu.VMEM((2, NX, HD), F32),
                DMA((2, G, 3)), DMA((2, 3)), DMA((2, 2, 3)), DMA((2, 3)), DMA((4, ONE + FIX))], 3,
        )(o1, st1, r1, g_mlp, g_final[None, :], *weights, w_vocab, one_r0, fix0)

        rest0, log_z = lax.optimization_barrier((rest0, log_z))
        rest_r0, rest_p0 = rest(bucket, rest0)
        ko, vo, cand = call(
            functools.partial(kernel_child, 0), 'assemble_first', 8, cache_out + [(shape((NB, G * VW), F32), HB)],
            [SM, SM, VM, VM, HB, VM] + [HB] * 12, child_scratch + [pltpu.VMEM(logits.shape, F32), pltpu.VMEM((NB, G * VW), F32), DMA((2,))], -1, ((16, 0), (17, 1)),
        )(meta, position, kv0, score1, logit, log_z, kc, vc, xp0, xq0, one_r0, one_p0, fix_r0, fix_p0, rest_r0, rest_p0, ko, vo)
        return ko.reshape(k_cache.shape), vo.reshape(v_cache.shape), cand

    in_specs = (row_spec, P('dp', None), full_rep, beam_spec, cache_spec, cache_spec) + (full_rep,) * 11
    return jax.shard_map(local_step, mesh=mesh, in_specs=in_specs, out_specs=(cache_spec, cache_spec, row_spec), check_vma=False)
```

```python
import functools

import jax
import jax.numpy as jnp
from jax import lax
from jax.experimental import pallas as pl
from jax.experimental.pallas import tpu as pltpu
from jax.sharding import PartitionSpec as P

ROPE_BASE, NORM_EPS, NEG = 10000.0, 1e-6, -1e30
MESH = pl.DeviceIdType.MESH
F32, BF16, I32 = jnp.float32, jnp.bfloat16, jnp.int32
G = 4
NB, NX, NA = 8, 16, 32
KVH, HD, HALF = 8, 128, 64
D, ROWS, SLOTS = 4096, 2048, 256
QW, KW, FW, VW = 1024, 256, 3584, 8192
QKV = QW + 2 * KW
FEW, MANY = 6, 20
TR, TC = 2048, 512
HT = 2
UT, UC = 7, 28
ONE, FIXES = 1, (3, 4, 5)
FIX = FIXES[-1]
ALL = ONE + FIX
SRC = 6
REST = NX - ALL
BUCKETS = (0, 1, 2, 4, 10)
SCALE = HD ** -0.5
EXP2 = SCALE * 1.4426950408889634
VM = pl.BlockSpec(memory_space=pltpu.VMEM)
HB = pl.BlockSpec(memory_space=pl.ANY)
SM = pl.BlockSpec(memory_space=pltpu.SMEM)
ROW = (ROWS, HD)
T_ORDER, T_START, T_COUNT, T_LIST, T_CODE, T_IDX, T_MISC, T_PAR = range(8)
DMA = pltpu.SemaphoreType.DMA


def coords():
    beam = lax.axis_index('beam')
    return beam // 2, lax.axis_index('sp'), beam % 2


def peer(x, y, c):
    return {'sp': y, 'beam': 2 * x + c}


def group_peers(x, y, c):
    return [(y, 1 - c), (1 - y, c), (1 - y, 1 - c)]


def all_peers(x, y, c):
    far = [(1 - x, yy, cc) for yy in (y, 1 - y) for cc in (c, 1 - c)]
    return far + [(x, yy, cc) for yy, cc in group_peers(x, y, c)]


def barrier_with(ids):
    sem = pltpu.get_barrier_semaphore()
    for dev in ids:
        pl.semaphore_signal(sem, inc=1, device_id=dev, device_id_type=MESH)
    pl.semaphore_wait(sem, len(ids))


def remote(src, dst, send_sem, recv_sem, dev):
    return pltpu.make_async_remote_copy(src_ref=src, dst_ref=dst, send_sem=send_sem, recv_sem=recv_sem,
                                        device_id=dev, device_id_type=MESH)


def ends(sem, *at):
    return sem.at[(0,) + at], sem.at[(1,) + at]


def local(src, dst, sem):
    return pltpu.make_async_copy(src, dst, sem)


def span(i, size):
    return pl.ds(pl.multiple_of(i * size, size), size)


def cols(i, size):
    return slice(i * size, (i + 1) * size)


def rsum(v):
    return jnp.sum(v, axis=-1, keepdims=True)


def rmax(v):
    return jnp.max(v, axis=-1, keepdims=True)


def csum(v):
    return jnp.sum(v, axis=0, keepdims=True)


def iota(shape_, dim):
    return lax.broadcasted_iota(I32, shape_, dim)


def mm(a, b):
    return jnp.dot(a, b, preferred_element_type=F32)


def start_all(copies):
    for cp in copies:
        cp.start()
    return copies


def wait_all(copies):
    for cp in copies:
        cp.wait()


class Stream:
    def __init__(self, wbuf, wsem, phases, ref_like):
        self.wbuf, self.wsem, self.like, self.depth = wbuf, wsem, ref_like, wbuf.shape[0]
        self.phases, base = [], 0
        for count, issue in phases:
            self.phases.append((base, count, issue))
            base += count
        self.total = base

    def issue(self, t, slot, lo, hi):
        for base, count, fetch in self.phases:
            if base + count <= lo or hi < base:
                continue
            if lo == hi or (base <= lo and hi < base + count):
                fetch(t - base, self.wbuf.at[slot], self.wsem.at[slot])
            else:
                @pl.when((t >= base) & (t < base + count))
                def _(base=base, fetch=fetch):
                    fetch(t - base, self.wbuf.at[slot], self.wsem.at[slot])

    def prologue(self):
        for t in range(min(self.depth, self.total)):
            self.issue(t, t, t, t)

    def run(self, phase, group, body):
        base, count, _ = self.phases[phase]

        @pl.loop(0, count // group)
        def _(i):
            first = i * group + base
            slots = [(first + k) % self.depth for k in range(group)]
            for slot in slots:
                local(self.like, self.wbuf.at[slot], self.wsem.at[slot]).wait()
            body(i, [self.wbuf.at[slot] for slot in slots])
            for k, slot in enumerate(slots):
                self.issue(first + k + self.depth, slot, base + self.depth, base + count - 1 + self.depth)


def col_tiles(w_ref, layer, g, width, row_chunks):
    def issue(i, buf, sem):
        ci, ri = i // row_chunks, i % row_chunks
        at = pl.ds(pl.multiple_of(g * width + ci * TC, TC), TC)
        src = w_ref.at[span(ri, TR), at] if layer < 0 else w_ref.at[layer, span(ri, TR), at]
        local(src, buf, sem).start()
    return issue


def kv_tiles(wk_ref, wv_ref, layer, g):
    def issue(i, buf, sem):
        for k, w_ref in enumerate((wk_ref, wv_ref)):
            local(w_ref.at[layer, span(i, TR), span(g, KW)], buf.at[:, pl.ds(k * KW, KW)], sem).start()
    return issue


def gate_up_tiles(wg_ref, wu_ref, layer, g):
    def issue(i, buf, sem):
        at = pl.ds(pl.multiple_of(g * FW + (i // G) * TC, TC), TC)
        for k, w_ref in enumerate((wg_ref, wu_ref)):
            @pl.when((i // HT) % 2 == k)
            def _():
                local(w_ref.at[layer, span(i % HT, TR), at], buf, sem).start()
    return issue


def norm_into(r_ref, g_row, hbuf):
    total = rsum(r_ref[0] * r_ref[0])
    for k in range(1, G):
        total = total + rsum(r_ref[k] * r_ref[k])
    inv = lax.rsqrt(total / D + NORM_EPS)
    for k in range(G):
        gain = g_row(cols(k, QW)).astype(F32)
        hbuf[k // 2, :, cols(k % 2, QW)] = (r_ref[k] * inv * gain).astype(BF16)


def rope(x_bf, cos_row, sin_row):
    v = x_bf.astype(F32)
    return (v * cos_row + pltpu.roll(v, HALF, 1) * sin_row).astype(BF16)


def stream_q(stream, part, hbuf, acc, cos_row, sin_row, out_ref, first=0):
    def body(i, w):
        acc[i + HT * part] = mm(hbuf[0], w[0][:]) + mm(hbuf[1], w[1][:])

    stream.run(first + part, HT, body)
    for head in (range(KVH), range(KVH, QKV // HD))[part]:
        piece = acc[head // G, :, cols(head % G, HD)].astype(BF16)
        if head * HD < QW + KW:
            piece = rope(piece, cos_row, sin_row)
        out_ref[:, cols(head, HD)] = piece


def my_half(piece, c):
    wide = piece.astype(F32)
    return jnp.where(c == 0, wide[:NB], wide[NB:])


def spread_kv(buf, base, c, out_ref, at):
    for k in range(G):
        for j in range(G):
            part, h = j // 2, j % 2
            out_ref[:, at + part * KVH + 2 * k + h, :] = my_half(buf[base + k, :, QW + j * HD:QW + (j + 1) * HD], c)


def own_start(buf, g, sems, k0, peers, x):
    return start_all([remote(buf.at[g], buf.at[g], *ends(sems, k0, k), peer(x, *p))
                      for k, p in enumerate(peers)])


def kernel_table(par_ref, meta_ref, choice_ref, bucket_ref):
    square = (NA, NA)
    i, j = iota(square, 0), iota(square, 1)
    par_row = jnp.broadcast_to(par_ref[:], square)
    par_col = rsum(jnp.where(i == j, par_row, 0).astype(F32)).astype(I32)
    fi, fj = i.astype(F32), j.astype(F32)

    def flag(v):
        return jnp.where(v, 1.0, 0.0)

    same, same_t = par_col == j, par_row == i
    far, half = (i // NX) != (j // NX), (i // NX) == (j // NX)
    before = rsum(flag((par_row < par_col) | ((par_row == par_col) & (j < i))))
    cross_row = jnp.minimum(csum(flag(same & far)), 1.0)
    cross_col = jnp.minimum(rsum(flag(same_t & far)), 1.0)
    place_col = rsum(flag(half & (j < i)) * cross_row)
    slot_col = place_col + (i // NX * NX).astype(F32)[:, :1]
    code = jnp.where(par_row // NB == j // NB, 0.0, jnp.where(par_row // NX == j // NX, 1.0, 2.0))[:1]
    place_par = csum(flag(same_t) * place_col)
    lane = j[:1]
    used = [rsum(jnp.where(lane // NX == k, cross_row, 0.0)) for k in range(2)]
    extra = jnp.maximum(used[0], used[1]) - ALL
    most = extra + FIX
    bucket = flag(extra > BUCKETS[0])
    choice = flag(most > FIXES[0]) + flag(most > FIXES[1])
    choice_ref[0] = choice.astype(I32)[0, 0]
    for n in BUCKETS[1:]:
        bucket = bucket + flag(extra > n)
    bucket_ref[0] = bucket.astype(I32)[0, 0]
    misc = jnp.where(lane == 0, used[0], used[1])
    rows = [csum(jnp.where(before == fj, fi, 0.0)), csum(flag(par_col < j)), csum(flag(same)),
            csum(jnp.where(slot_col == fj, fi, 0.0) * cross_col), code,
            jnp.where(code > 1.0, place_par, (par_row % NB).astype(F32)[:1]), misc, par_row[:1].astype(F32)]
    for k, row in enumerate(rows):
        meta_ref[k:k + 1, :NA] = row.astype(I32)


def kernel_a(tok_ref, score_ref, cos_ref, sin_ref, ga_ref, wq_ref, wk_ref, wv_ref, k_ref, v_ref,
             q_out, kv_out, own_out, r_out, score_out, xp_out,
             wbuf, wsem, tokx, scx, r_s, hbuf, acc, qkvx, ssem, rsem, xsem):
    x, y, c = coords()
    g = y * 2 + c
    d = x * G + g
    stream = Stream(wbuf, wsem, [(G, col_tiles(wq_ref, 0, g, QW, HT)), (HT, kv_tiles(wk_ref, wv_ref, 0, g))],
                    wq_ref.at[0, pl.ds(0, TR), pl.ds(0, TC)])
    stream.prologue()
    others = all_peers(x, y, c)
    barrier_with([peer(*p) for p in others])
    tok_copy = remote(tok_ref, tokx, ssem.at[0], rsem.at[0], peer(x, y, 1 - c))
    tok_copy.start()
    beam = 2 * x + c
    for i in range(NB):
        scx[beam, i:i + 1, :] = jnp.full((1, HD), score_ref[i], F32)
    for k in range(G):
        r_s[k, span(c, NB), :] = tok_ref[:, cols(k, QW)].astype(F32)
    sc_copies = start_all([remote(scx.at[beam], scx.at[beam], ssem.at[k], rsem.at[k], peer(xx, y, cc))
                           for k, (xx, cc) in enumerate(((1 - x, c), (1 - x, 1 - c), (x, 1 - c)), 1)])
    beside = peer(x, y, 1 - c)
    for k, ref in enumerate((k_ref, v_ref)):
        @pl.when(1 - c == k)
        def _():
            @pl.loop(0, NB)
            def _(r):
                remote(ref.at[1, r], xp_out.at[r], xsem.at[0], xsem.at[1], beside).start()

    tok_copy.wait()
    for k in range(G):
        r_s[k, span(1 - c, NB), :] = tokx[:, cols(k, QW)].astype(F32)
    norm_into(r_s, lambda at: ga_ref[0:1, at], hbuf)
    for i in range(HT):
        stream_q(stream, i, hbuf, acc, cos_ref[:], sin_ref[:], qkvx.at[d])
        own = qkvx.at[d]
        piece = own.at[:, pl.ds(0, QW)] if i == 0 else own.at[:, pl.ds(QW, 2 * KW)]
        copies = start_all([remote(piece, piece, ssem.at[G * (i + 1) + k], rsem.at[G * (i + 1) + k], peer(*p))
                            for k, p in enumerate(others) if i == 0 or k >= G])
        if i == 0:
            q_copies = copies
    own_out[:] = qkvx[d]
    r_out[:] = r_s[:]
    wait_all(sc_copies)
    for k in range(G):
        score_out[cols(k, NB), :] = scx[k]

    def spread_q(dd):
        for h in range(KVH):
            q_out[span(dd // G, NX), dd % G * KVH + h, :] = qkvx[dd, :, cols(h, HD)].astype(F32)

    spread_q(d)
    wait_all(copies)
    spread_kv(qkvx, x * G, c, kv_out, 0)
    for k in range(len(others) - 1, -1, -1):
        q_copies[k].wait()
        xx, yy, cc = others[k]
        spread_q(xx * G + yy * 2 + cc)
    remote(xp_out, xp_out, xsem.at[0], xsem.at[1], beside).wait()


def mask_bias(limit):
    row, col = iota((NA, ROWS), 0), iota((NA, ROWS), 1)
    ok = ((col % KVH) == (row // G)) & (col < limit * KVH)
    return jnp.where(ok, 0.0, NEG)


def attend(q, k_rows, v_rows, bias):
    s = lax.dot_general(q, k_rows, (((1,), (1,)), ((), ())), preferred_element_type=F32)
    s = (s.reshape(-1, NA, ROWS) + bias[:]).reshape(s.shape)
    m = rmax(s)
    e = jnp.exp2((s - m) * EXP2)
    return mm(e.astype(BF16), v_rows), m * SCALE, rsum(e)


def to_lanes(column):
    return csum(jnp.where(iota((NA, HD), 0) == iota((NA, HD), 1), column, 0.0))


def keep(o_ref, st_ref, b, o, m, total):
    o_ref[b] = o
    st_ref[0, pl.ds(b, 1), :] = to_lanes(m)
    st_ref[1, pl.ds(b, 1), :] = to_lanes(total)


def kernel_home(meta, pos_ref, q_ref, k_ref, v_ref, o_ref, st_ref, kbuf, vbuf, bias, ksem, vsem):
    x, y, c = coords()
    first = (2 * x + c) * NB
    limit = jnp.clip(pos_ref[0] - y * SLOTS, 0, SLOTS)

    def count_of(r):
        return jnp.where(limit > 0, meta[T_COUNT, first + r], 0)

    def copies(r):
        return local(k_ref.at[0, r], kbuf.at[r], ksem.at[r]), local(v_ref.at[0, r], vbuf.at[r], vsem.at[r])

    @pl.loop(0, NB)
    def _(r):
        @pl.when(count_of(r) > 0)
        def _():
            start_all(copies(r))

    o_ref[:] = jnp.zeros_like(o_ref)
    st_ref[0] = jnp.full((NA, HD), NEG, F32)
    st_ref[1] = jnp.zeros((NA, HD), F32)
    bias[:] = mask_bias(limit)

    @pl.loop(0, NB)
    def _(r):
        count = count_of(r)
        start = meta[T_START, first + r]

        @pl.when(count > 0)
        def _():
            wait_all(copies(r))

        def step(s, carry):
            beams = [meta[T_ORDER, start + jnp.minimum(s * G + j, count - 1)] for j in range(G)]
            q = jnp.concatenate([q_ref[b] for b in beams], axis=0).astype(BF16)
            o, m, total = attend(q, kbuf[r], vbuf[r], bias)
            for j, b in enumerate(beams):
                at = cols(j, NA)
                keep(o_ref, st_ref, b, o[at], m[at], total[at])
            return carry

        lax.fori_loop(0, (count + G - 1) // G, step, 0)


def lane_pick(rows, lane):
    return rsum(jnp.where(iota(rows.shape, 1) == lane, rows, 0.0))


def send_partials(o_ref, st_ref, ox, sx, om, sm, x, y, c, psem):
    g = y * 2 + c
    far = span(1 - x, NX)
    beside = peer(x, y, 1 - c)
    merge = [remote(st_ref.at[:, far, :], sm, *ends(psem, 0, 0), beside)]
    for yy in range(2):
        merge.append(remote(o_ref.at[far, span(yy * 2 + 1 - c, KVH), :], om.at[yy], *ends(psem, 1, yy), beside))
    start_all(merge)
    near, copies = span(x, NX), []
    for k, (yy, cc) in enumerate(group_peers(x, y, c), 2):
        dev = peer(x, yy, cc)
        copies.append(remote(st_ref.at[:, near, :], sx.at[g], *ends(psem, 0, k), dev))
        copies.append(remote(o_ref.at[near, span(yy * 2 + cc, KVH), :], ox.at[g], *ends(psem, 1, k), dev))
    start_all(copies)
    sx[g] = st_ref[:, near, :]
    ox[g] = o_ref[near, span(g, KVH), :]
    wait_all(merge)
    sm[0] = jnp.maximum(sm[0], st_ref[0, far, :])
    sm[1] = sm[1] + st_ref[1, far, :]
    for yy in range(2):
        om[yy] = om[yy] + o_ref[far, span(yy * 2 + c, KVH), :]
    across = []
    for k, dy in enumerate((0, 1), 5):
        yy = (y + dy) % 2
        dev = peer(1 - x, yy, c)
        across.append(remote(sm, sx.at[G + y], *ends(psem, 0, k), dev))
        across.append(remote(om.at[yy], ox.at[G + y], *ends(psem, 1, k), dev))
    return copies + start_all(across)


def combine_first(copies, own_ref, ox, sx, g, out_ref):
    lanes = iota((NX, HD), 1)
    s_self = jnp.full((NX, HD), NEG, F32)
    for h in range(KVH):
        q = own_ref[:, cols(h, HD)].astype(F32)
        kk = own_ref[:, cols(KVH + h // G, HD)].astype(F32)
        s_self = jnp.where(lanes == g * KVH + h, rsum(q * kk) * SCALE, s_self)
    wait_all(copies)
    top = s_self
    for i in range(SRC):
        top = jnp.maximum(top, sx[i, 0])
    e_self = jnp.exp(s_self - top)
    total = e_self
    weights = []
    for i in range(SRC):
        weights.append(jnp.exp(sx[i, 0] - top))
        total = total + weights[i] * sx[i, 1]
    for h in range(KVH):
        lane = g * KVH + h
        vv = own_ref[:, cols(KVH + 2 + h // G, HD)].astype(F32)
        mix = lane_pick(e_self, lane).astype(BF16).astype(F32) * vv
        for i in range(SRC):
            mix = mix + lane_pick(weights[i], lane) * ox[i, :, h, :]
        out_ref[:, cols(h, HD)] = (mix / lane_pick(total, lane)).astype(BF16)


class Crossing:
    def __init__(self, x, y, c, rows, sems):
        self.first, self.second = [], []
        for k, (src, got, passed) in enumerate(rows):
            if src is not got:
                self.first.append(remote(src, got, *ends(sems, k), peer(1 - x, y, c)))
            self.second.append(remote(got, passed, sems.at[2, k], sems.at[3, k], peer(x, y, 1 - c)))
        self.ready = len(self.second) - len(self.first)

    def start(self):
        start_all(self.first)
        start_all(self.second[:self.ready])

    def forward(self, k):
        self.first[k].wait_recv()
        self.second[self.ready + k].start()

    def finish(self, k):
        for i in range(k, len(self.first)):
            self.forward(i)
        for cp in self.first:
            cp.wait_send()
        wait_all(self.second)


def fix_rows(n, fix_ref, fix_r, fix_p):
    return [(fix_ref.at[k], fix_r.at[k], fix_p.at[k]) for k in range(n)]


def out_mlp(stream, first, g, x, peers, r_s, hbuf, acc, ox, yx, zx, ubuf, gm_row, sems, usem, cross, side):
    def half_sends(buf, k0, i):
        buf[g, i] = acc[i].astype(BF16)
        start_all([remote(buf.at[g, i], buf.at[g, i], *ends(sems, k0, k), peer(x, *p))
                   for k, p in enumerate(peers)])

    def add(buf, k0):
        wait_all([remote(buf.at[g], buf.at[g], *ends(sems, k0, k), peer(x, *p)) for k, p in enumerate(peers)])
        for k in range(G):
            for i in range(HT):
                r_s[k, :, cols(i, TC)] = r_s[k, :, cols(i, TC)] + buf[k, i].astype(F32)

    copies = own_start(ox, g, sems, 0, peers, x)
    wait_all(copies)
    for k in range(G):
        hbuf[k // 2, :, cols(k % 2, QW)] = ox[k]

    def project(w):
        return mm(hbuf[0], w[0][:]) + mm(hbuf[1], w[1][:])

    def body_out(i, w):
        acc[i] = project(w)
        half_sends(yx, 1, i)

    stream.run(first, HT, body_out)
    add(yx, 1)
    norm_into(r_s, gm_row, hbuf)

    def body_gu(i, w):
        side(6 + 2 * i, KVH + 2 * i)
        gate = project(w[:HT]).astype(BF16).astype(F32)
        up = project(w[HT:]).astype(BF16).astype(F32)
        at = g * UT + i
        ubuf[at] = (jax.nn.silu(gate) * up).astype(BF16)
        start_all([remote(ubuf.at[at], ubuf.at[at], *ends(usem, k), peer(x, *p))
                   for k, p in enumerate(peers)])

    stream.run(first + 1, G, body_gu)
    cross.forward(0)
    mine = ubuf.at[pl.ds(g * UT, UT)]
    wait_all([remote(mine, mine, *ends(usem, k), peer(x, *p)) for k, p in enumerate(peers)])

    def body_down(i, w):
        side(20 + G * i, G * 6)
        total = mm(ubuf[0], w[0][cols(0, TC), :])
        for k in range(1, UC):
            total = total + mm(ubuf[k], w[k // G][cols(k % G, TC), :])
        acc[i] = total
        half_sends(zx, 2, i)

    stream.run(first + 2, UT, body_down)
    add(zx, 2)


def mlp_phases(layer, g, wo_ref, wg_ref, wu_ref, wd_ref):
    return [(G, col_tiles(wo_ref, layer, g, QW, HT)),
            (UC, gate_up_tiles(wg_ref, wu_ref, layer, g)),
            (2 * UT, col_tiles(wd_ref, layer, g, QW, UT))]


def kernel_mid(n, o_ref, st_ref, own_ref, r_ref, cos_ref, sin_ref, ga_ref, gm_ref, wo_ref, wg_ref, wu_ref, wd_ref, wq_ref, wk_ref, wv_ref,
               k_ref, v_ref, one_ref, fix_ref,
               qkv_out, r_out, one_p, fix_r, fix_p, xq1_out, xp0_out, xq0_out,
               wbuf, wsem, r_s, hbuf, acc, ox, yx, zx, ubuf, qkvx, px, sx, om, sm, sems, usem, csem, xsem, psem):
    x, y, c = coords()
    g = y * 2 + c
    peers = group_peers(x, y, c)
    stream = Stream(wbuf, wsem, mlp_phases(0, g, wo_ref, wg_ref, wu_ref, wd_ref) + [
        (G, col_tiles(wq_ref, 1, g, QW, HT)), (HT, kv_tiles(wk_ref, wv_ref, 1, g))],
        wq_ref.at[0, pl.ds(0, TR), pl.ds(0, TC)])
    stream.prologue()
    beside = peer(x, y, 1 - c)
    others = all_peers(x, y, c)
    barrier_with([peer(*p) for p in others])
    here = one_ref.at[0]
    cross = Crossing(x, y, c, [(here, here, one_p.at[0])] + fix_rows(n, fix_ref, fix_r, fix_p), csem)
    partials = send_partials(o_ref, st_ref, px, sx, om, sm, x, y, c, psem)
    cross.start()
    r_s[:] = r_ref[:]

    others_rows = ((1, c, xq1_out), (0, 1 - c, xp0_out), (0, c, xq0_out))

    def side(lo, hi):
        @pl.loop(lo, hi)
        def _(q):
            for at, (layer, part, out) in enumerate(others_rows):
                for k, ref in enumerate((k_ref, v_ref)):
                    @pl.when((q // NB == at) & (part == k))
                    def _():
                        remote(ref.at[layer, q % NB], out.at[q % NB], *ends(xsem, at), beside).start()

    side(0, 6)
    combine_first(partials, own_ref, px, sx, g, ox.at[g])
    out_mlp(stream, 0, g, x, peers, r_s, hbuf, acc, ox, yx, zx, ubuf, lambda at: gm_ref[0:1, at], sems, usem, cross, side)
    cross.forward(1)
    norm_into(r_s, lambda at: ga_ref[1:2, at], hbuf)
    for i in range(HT):
        stream_q(stream, i, hbuf, acc, cos_ref[:], sin_ref[:], qkvx.at[g], 3)
        own = qkvx.at[g]
        piece = own.at[:, pl.ds(0, QW)] if i == 0 else own.at[:, pl.ds(QW, 2 * KW)]
        copies = start_all([remote(piece, piece, *ends(sems, 3 * i, k), peer(x, *p)) for k, p in enumerate(peers)])
        if i == 0:
            q_copies = copies
    cross.forward(2)
    r_out[:] = r_s[:]
    for k, (_, _, out) in enumerate(others_rows):
        remote(out, out, *ends(xsem, k), beside).wait()
    wait_all(q_copies + copies)
    for k in range(G):
        for h in range(KVH):
            qkv_out[:, k * KVH + h, :] = my_half(qkvx[k, :, cols(h, HD)], c)
    spread_kv(qkvx, 0, c, qkv_out, NA)
    cross.finish(3)


def kernel_end(n, o_ref, st_ref, r_ref, gm_ref, gf_ref, wo_ref, wg_ref, wu_ref, wd_ref, wvoc_ref,
               fix_ref,
               candx, log_out, fix_r, fix_p,
               wbuf, wsem, r_s, hbuf, acc, ox, yx, zx, ubuf, px, sx, lbuf, stx, run_st,
               sems, usem, psem, lsem, csem):
    x, y, c = coords()
    g = y * 2 + c
    peers = group_peers(x, y, c)
    stream = Stream(wbuf, wsem, mlp_phases(1, g, wo_ref, wg_ref, wu_ref, wd_ref) + [
        (VW // TC * HT, col_tiles(wvoc_ref, -1, g, VW, HT))],
        wvoc_ref.at[pl.ds(0, TR), pl.ds(0, TC)])
    stream.prologue()
    barrier_with([peer(x, *p) for p in peers] + [peer(1 - x, y, c)])
    cross = Crossing(x, y, c, fix_rows(n + ONE, fix_ref, fix_r, fix_p), csem)
    cross.start()
    copies = []
    for k, (yy, cc) in enumerate(peers):
        heads, dev = span(yy * 2 + cc, KVH), peer(x, yy, cc)
        copies.append(remote(st_ref, sx.at[g], *ends(psem, 0, k), dev))
        copies.append(remote(o_ref.at[:, heads, :], px.at[g], *ends(psem, 1, k), dev))
    start_all(copies)
    sx[g] = st_ref[:]
    px[g] = o_ref[:, span(g, KVH), :]
    r_s[:] = r_ref[:]
    wait_all(copies)
    for cc in range(2):
        pair = (cc, 2 + cc)
        top = jnp.maximum(sx[pair[0], 0], sx[pair[1], 0])
        weights = [jnp.exp(sx[p, 0] - top) for p in pair]
        total = weights[0] * sx[pair[0], 1] + weights[1] * sx[pair[1], 1]
        for h in range(KVH):
            lane = g * KVH + h
            mix = lane_pick(weights[0], lane) * px[pair[0], :, h, :] + lane_pick(weights[1], lane) * px[pair[1], :, h, :]
            acc[h // G, cols(cc, NB), cols(h % G, HD)] = mix / lane_pick(total, lane)
    for k in range(HT):
        ox[g, :, cols(k, TC)] = acc[k].astype(BF16)
    out_mlp(stream, 0, g, x, peers, r_s, hbuf, acc, ox, yx, zx, ubuf, lambda at: gm_ref[1:2, at], sems, usem, cross, lambda lo, hi: lo)
    cross.forward(1)
    norm_into(r_s, lambda at: gf_ref[at].reshape(1, QW), hbuf)
    run_st[0] = jnp.full((NX, HD), NEG, F32)
    run_st[1] = jnp.zeros((NX, HD), F32)
    nv = VW // TC

    def body_voc(i, w):
        logits = mm(hbuf[0], w[0][:]) + mm(hbuf[1], w[1][:])
        for cc in range(2):
            lbuf[i, cc] = logits[cols(cc, NB)]
        at = g * nv + i
        candx[at] = lbuf[i, c]
        start_all([remote(lbuf.at[i, cc], candx.at[at], *ends(lsem, k), peer(x, yy, cc))
                   for k, (yy, cc) in enumerate(peers)])
        @pl.when(i == nv // 2)
        def _():
            cross.forward(2)

        old = run_st[0][:, :1]
        top = jnp.maximum(old, rmax(logits))
        run_st[1] = run_st[1] * jnp.exp(old - top) + rsum(jnp.exp(logits - top))
        run_st[0] = jnp.broadcast_to(top, (NX, HD))

    stream.run(3, HT, body_voc)
    stx[g] = run_st[:]
    wait_all(own_start(stx, g, sems, 3, peers, x))
    tops = [stx[k, 0, span(c, NB), :] for k in range(G)]
    top = functools.reduce(jnp.maximum, tops)
    total = sum(stx[k, 1, span(c, NB), :] * jnp.exp(tops[k] - top) for k in range(G))
    log_out[:] = top + jnp.log(total)
    got = candx.at[pl.ds(g * nv, nv)]
    wait_all([remote(lbuf.at[:, cc], got, *ends(lsem, k), peer(x, yy, cc)) for k, (yy, cc) in enumerate(peers)])
    cross.finish(3)


class Pack:
    def __init__(self, layer, meta, k_ref, v_ref, xp_ref, segments, buf, isem, osem):
        self.x, _, self.c = coords()
        self.layer, self.meta, self.own, self.xp = layer, meta, (k_ref, v_ref), xp_ref
        self.segments, self.buf, self.isem, self.osem = segments, buf, isem, osem

    def each(self, fn):
        lax.fori_loop(0, self.meta[T_MISC, self.x], lambda p, z: (fn(p), z)[1], 0)

    def fetch(self):
        self.each(self.fetch_one)

    def fetch_one(self, p):
        v = self.meta[T_LIST, self.x * NX + p]
        r, own = v % NB, (v // NB) % 2 == self.c
        for core, mine in enumerate(self.own):
            @pl.when((self.c == core) & own)
            def _():
                local(mine.at[self.layer, r], self.buf.at[p], self.isem.at[p]).start()

        @pl.when(jnp.logical_not(own))
        def _():
            local(self.xp.at[r], self.buf.at[p], self.isem.at[p]).start()

    def store(self, p, op):
        for ref, lo, hi in self.segments:
            @pl.when((p >= lo) & (p < hi))
            def _():
                op(local(self.buf.at[p], ref.at[jnp.clip(p - lo, 0, hi - lo - 1)], self.osem.at[p]))

    def move(self):
        def one(p):
            local(self.xp.at[0], self.buf.at[p], self.isem.at[p]).wait()
            self.store(p, lambda cp: cp.start())
        self.each(one)

    def finish(self):
        self.each(lambda p: self.store(p, lambda cp: cp.wait()))


def kernel_pack(meta, dep, k_ref, v_ref, xp_ref, one, fix, rest, buf, isem, osem):
    pack = Pack(1, meta, k_ref, v_ref, xp_ref, ((one, 0, ONE), (fix, ONE, ALL), (rest, ALL, NX)), buf, isem, osem)
    pack.fetch()
    pack.move()
    pack.finish()


def fetch_row(layer, meta, b, mine, own_ref, partner, crossed, dst, sem):
    code, idx = meta[T_CODE, b], meta[T_IDX, b]

    @pl.when(code == 0)
    def _():
        local(own_ref.at[layer, idx % NB], dst, sem).start()

    for ref, cond in zip(partner, (mine, jnp.logical_not(mine))):
        @pl.when((code == 1) & cond)
        def _():
            local(ref.at[idx % NB], dst, sem).start()

    for lo, hi, refs in crossed:
        for ref, cond in zip(refs, (mine, jnp.logical_not(mine))):
            @pl.when((code == 2) & (idx >= lo) & (idx < hi) & cond)
            def _():
                local(ref.at[jnp.clip(idx - lo, 0, hi - lo - 1)], dst, sem).start()


def put_new(buf, i, new, at):
    rows = span(at // 2, NX)
    hit = iota((NX, HD), 0) // KVH == at % 2
    both = jnp.concatenate([new, new], axis=0)
    buf[i, rows, :] = jnp.where(hit, both, buf[i, rows, :].astype(F32)).astype(BF16)


def kernel_child(layer, *refs):
    if layer:
        (meta, pos_ref, new_ref, score_ref, k_ref, v_ref, xp, xq, one_r, one_p, fix_r, fix_p, rest_r, rest_p, xp0,
         ko, vo, o_ref, st_ref, score_out, fix0, rest0, kbuf, vbuf, isem, osem, bias, pbuf, pisem, posem) = refs
        crossed = ((0, ONE, (one_r, one_p)), (ONE, ALL, (fix_r, fix_p)), (ALL, NX, (rest_r, rest_p)))
        pack = Pack(0, meta, k_ref, v_ref, xp0, ((fix0, 0, ALL), (rest0, ALL, NX)), pbuf, pisem, posem)
        at0 = NA
    else:
        (meta, pos_ref, new_ref, score_ref, logits_ref, log_ref, k_ref, v_ref, xp, xq, fix_r, fix_p, rest_r, rest_p, _, _,
         ko, vo, cand_ref, kbuf, vbuf, isem, osem, logit_buf, cand_buf, csem) = refs
        at0 = 0
        crossed = ((0, ALL, (fix_r, fix_p)), (ALL, NX, (rest_r, rest_p)))
        logits_in = local(logits_ref, logit_buf, csem.at[0])
        logits_in.start()
    x, y, c = coords()
    first = (2 * x + c) * NB
    pos = pos_ref[0] - y * SLOTS
    both = ((k_ref, kbuf, ko), (v_ref, vbuf, vo))

    @pl.loop(0, NB)
    def _(i):
        for part, (src, buf, _) in enumerate(both):
            fetch_row(layer, meta, first + i, c == part, src, (xp, xq), crossed, buf.at[i], isem.at[part, i])

    if layer:
        pack.fetch()
        bias[:] = mask_bias(jnp.clip(pos + 1, 1, SLOTS))
    else:
        logits_in.wait()

    @pl.loop(0, NB)
    def _(i):
        for part, (src, buf, out) in enumerate(both):
            local(src.at[0, 0], buf.at[i], isem.at[part, i]).wait()

            @pl.when((pos >= 0) & (pos < SLOTS))
            def _():
                start = at0 + part * KVH
                put_new(buf, i, new_ref[i, start:start + KVH, :], jnp.clip(pos, 0, SLOTS - 1))

            local(buf.at[i], out.at[layer, i], osem.at[part, i]).start()
        if not layer:
            for k in range(KVH):
                at = i * KVH + k
                cand_buf[:, span(at, TC)] = score_ref[:, :1] + (logit_buf[at] - log_ref[:, :1])
            local(cand_buf.at[:, span(i, D)], cand_ref.at[:, span(i, D)], csem.at[1]).start()
        if layer:
            keep(o_ref, st_ref, i, *attend(new_ref[i, :NA, :].astype(BF16), kbuf[i], vbuf[i], bias))
            score_out[pl.ds(i, 1), :] = score_ref[pl.ds(meta[T_PAR, first + i], 1), :]

    if layer:
        pack.move()

    @pl.loop(0, NB)
    def _(i):
        for part, (_, buf, out) in enumerate(both):
            local(buf.at[i], out.at[layer, i], osem.at[part, i]).wait()

    if layer:
        pack.finish()
    else:
        local(cand_buf, cand_ref, csem.at[1]).wait()


def kernel_rest(n, src, got, passed, sems):
    x, y, c = coords()
    barrier_with([peer(1 - x, y, c), peer(x, y, 1 - c)])
    cross = Crossing(x, y, c, [(src.at[i], got.at[i], passed.at[i]) for i in range(n)], sems)
    cross.start()
    cross.finish(0)


def shape(s, t=BF16):
    return jax.ShapeDtypeStruct(s, t)


def rows_of(n):
    return shape((n,) + ROW)


def scratch_stream(n=MANY):
    return [pltpu.VMEM((n, TR, TC), BF16), DMA((n,))]


def scratch_mlp():
    wide = (G, NX, QW)
    return [pltpu.VMEM(wide, F32), pltpu.VMEM((HT, NX, TR), BF16), pltpu.VMEM((HT + 1, NX, TC), F32),
            pltpu.VMEM(wide, BF16), pltpu.VMEM((G, HT, NX, TC), BF16), pltpu.VMEM((G, HT, NX, TC), BF16),
            pltpu.VMEM((UC, NX, TC), BF16)]


def call(kernel, name, us, outs, ins, scratch, cid=-1, aliases=()):
    more = {} if cid < 0 else dict(collective_id=cid, has_side_effects=True)
    return pl.pallas_call(
        kernel, out_shape=tuple(o for o, _ in outs), in_specs=ins, out_specs=tuple(s for _, s in outs),
        scratch_shapes=scratch, input_output_aliases=dict(aliases), name=name,
        cost_estimate=pl.CostEstimate(flops=us * 400000000, bytes_accessed=us * 3000000, transcendentals=0),
        compiler_params=pltpu.CompilerParams(vmem_limit_bytes=123 * 2 ** 19, **more))


def solution(mesh):
    beam_spec = P(('dp', 'beam'))
    row_spec = P(('dp', 'beam'), None)
    cache_spec = P(None, ('dp', 'beam'), 'sp', None, None)
    full_rep = P()
    swap_x = [(b, (b + 2) % G) for b in range(G)]

    def rest(index, packed):
        def branch(k, n):
            outs = [(rows_of(REST), HB)] * 2
            if n == 0:
                return call(lambda *_: None, 'rest_none', 1, outs, [HB], [])
            return call(functools.partial(kernel_rest, n), f'rest_{n}', 1, outs, [HB], [DMA((4, n))], NX + k)
        return lax.switch(index, [branch(k, n) for k, n in enumerate(BUCKETS)], packed)

    def local_step(tok_emb, parent, position, beam_score, k_cache, v_cache, w_query, w_key, w_value, w_out, w_gate, w_up, w_down, g_attn, g_mlp, g_final, w_vocab):
        cur_pos = position[0]
        half = jnp.arange(HD, dtype=I32) % HALF
        inv_freq = ROPE_BASE ** (-2.0 * half.astype(F32) / HD)
        angles = (cur_pos.astype(F32) * inv_freq)[None, :]
        cos_row = jnp.cos(angles)
        sin_row = jnp.sin(angles) * jnp.where(jnp.arange(HD) < HALF, -1.0, 1.0)
        kc, vc = k_cache.reshape((2, NB) + ROW), v_cache.reshape((2, NB) + ROW)
        lanes = shape((NA, HD), F32)
        logits = shape((G * VW // TC, NB, TC), F32)

        meta, choice, bucket = call(kernel_table, 'table', 2, [(shape((NB, HD), I32), VM), (shape((1,), I32), SM), (shape((1,), I32), SM)], [VM], [])(parent)
        choice, bucket = choice.reshape(()), bucket.reshape(())

        def chosen(kernel, name, us, outs, ins, scratch, cid):
            return lambda *args: lax.switch(choice, [
                call(functools.partial(kernel, n), f'{name}_{n}', us, outs, ins, scratch, cid + n) for n in FIXES], *args)

        q0, kv0, own0, r0, scores, xp1 = call(
            kernel_a, 'qkv_first', 12,
            [(shape((NA, NA, HD), F32), VM), (shape((NB, NX, HD), F32), VM), (shape((NX, QKV)), VM),
             (shape((G, NX, QW), F32), VM), (lanes, VM), (rows_of(NB), HB)],
            [VM, SM, VM, VM, VM] + [HB] * 5,
            scratch_stream(FEW) + [
                pltpu.VMEM((NB, D), BF16), pltpu.VMEM((G, NB, HD), F32), pltpu.VMEM((G, NX, QW), F32),
                pltpu.VMEM((HT, NX, TR), BF16), pltpu.VMEM((HT + 1, NX, TC), F32), pltpu.VMEM((2 * G, NX, QKV), BF16),
                DMA((G * G,)), DMA((G * G,)), DMA((2,))], 1,
        )(tok_emb, beam_score, cos_row, sin_row, g_attn, w_query, w_key, w_value, kc, vc)

        pack_scratch = [pltpu.VMEM((NX,) + ROW, BF16), DMA((NX,)), DMA((NX,))]
        one1, fix1, rest1 = call(kernel_pack, 'pack_rows', 3, [(rows_of(ONE), HB), (rows_of(FIX), HB), (rows_of(REST), HB)],
                                 [SM] + [HB] * 4, pack_scratch)(meta, own0, kc, vc, xp1)
        one_r1 = lax.ppermute(one1, 'beam', swap_x)
        o0, st0 = call(
            kernel_home, 'attend_home', 9, [(shape((NA, NA, HD), F32), VM), (shape((2, NA, HD), F32), VM)],
            [SM, SM, VM, HB, HB],
            [pltpu.VMEM((NB,) + ROW, BF16)] * 2 + [pltpu.VMEM((NA, ROWS), F32), DMA((NB,)), DMA((NB,))],
        )(meta, position, q0, kc, vc)


        weights = (w_out, w_gate, w_up, w_down)
        qkv1, r1, one_p1, fix_r1, fix_p1, xq1, xp0, xq0 = chosen(
            kernel_mid, 'mlp_first', 50,
            [(shape((NB, NA + NX, HD), F32), VM), (shape((G, NX, QW), F32), VM), (rows_of(ONE), HB),
             (rows_of(FIX), HB), (rows_of(FIX), HB)] + [(rows_of(NB), HB)] * 3,
            [VM] * 8 + [HB] * 11,
            scratch_stream() + scratch_mlp() + [
                pltpu.VMEM((G, NX, QKV), BF16), pltpu.VMEM((SRC, NX, KVH, HD), F32), pltpu.VMEM((SRC, 2, NX, HD), F32),
                pltpu.VMEM((2, NX, KVH, HD), F32), pltpu.VMEM((2, NX, HD), F32), DMA((2, G, 3)), DMA((2, 3)), DMA((4, ALL)), DMA((2, 3)), DMA((2, 2, 7))], 0,
        )(o0, st0, own0, r0, cos_row, sin_row, g_attn, g_mlp, *weights, w_query, w_key, w_value, kc, vc, one_r1, fix1)

        rest1, _ = lax.optimization_barrier((rest1, r1))
        rest_r1, rest_p1 = rest(bucket, rest1)

        child_scratch = [pltpu.VMEM((NB,) + ROW, BF16), pltpu.VMEM((NB,) + ROW, BF16), DMA((2, NB)), DMA((2, NB))]
        cache_out = [(shape((2, NB) + ROW), HB)] * 2
        ko, vo, o1, st1, score1, fix0, rest0 = call(
            functools.partial(kernel_child, 1), 'attend_child', 9,
            cache_out + [(shape((NB, NA, HD), F32), VM), (shape((2, NB, HD), F32), VM), (shape((NB, HD), F32), VM),
                         (rows_of(ALL), HB), (rows_of(REST), HB)],
            [SM, SM, VM, VM] + [HB] * 11, child_scratch + [pltpu.VMEM((NA, ROWS), F32)] + pack_scratch,
        )(meta, position, qkv1, scores, kc, vc, xp1, xq1, one_r1, one_p1, fix_r1, fix_p1, rest_r1, rest_p1, xp0)

        logit, log_z, fix_r0, fix_p0 = chosen(
            kernel_end, 'mlp_vocab', 58,
            [(logits, VM), (shape((NB, HD), F32), VM), (rows_of(ALL), HB), (rows_of(ALL), HB)],
            [VM] * 5 + [HB] * 6,
            scratch_stream() + scratch_mlp() + [
                pltpu.VMEM((G, NB, KVH, HD), F32), pltpu.VMEM((G, 2, NB, HD), F32),
                pltpu.VMEM((VW // TC, 2, NB, TC), F32), pltpu.VMEM((G, 2, NX, HD), F32),
                pltpu.VMEM((2, NX, HD), F32),
                DMA((2, G, 3)), DMA((2, 3)), DMA((2, 2, 3)), DMA((2, 3)), DMA((4, ALL))], 3,
        )(o1, st1, r1, g_mlp, g_final, *weights, w_vocab, fix0)

        rest0, log_z = lax.optimization_barrier((rest0, log_z))
        rest_r0, rest_p0 = rest(bucket, rest0)
        ko, vo, cand = call(
            functools.partial(kernel_child, 0), 'assemble_first', 8, cache_out + [(shape((NB, G * VW), F32), HB)],
            [SM, SM, VM, VM, HB, VM] + [HB] * 10, child_scratch + [pltpu.VMEM(logits.shape, F32), pltpu.VMEM((NB, G * VW), F32), DMA((2,))], -1, ((14, 0), (15, 1)),
        )(meta, position, kv0, score1, logit, log_z, kc, vc, xp0, xq0, fix_r0, fix_p0, rest_r0, rest_p0, ko, vo)
        return ko.reshape(k_cache.shape), vo.reshape(v_cache.shape), cand

    in_specs = (row_spec, P('dp', None), full_rep, beam_spec, cache_spec, cache_spec) + (full_rep,) * 11
    return jax.shard_map(local_step, mesh=mesh, in_specs=in_specs, out_specs=(cache_spec, cache_spec, row_spec), check_vma=False)
```

```python
import functools

import jax
import jax.numpy as jnp
from jax import lax
from jax.experimental import pallas as pl
from jax.experimental.pallas import tpu as pltpu
from jax.sharding import PartitionSpec as P

ROPE_BASE, NORM_EPS, NEG = 10000.0, 1e-6, -1e30
MESH = pl.DeviceIdType.MESH
F32, BF16, I32 = jnp.float32, jnp.bfloat16, jnp.int32
G = 4
NB, NX, NA = 8, 16, 32
KVH, HD, HALF = 8, 128, 64
D, ROWS, SLOTS = 4096, 2048, 256
QW, KW, FW, VW = 1024, 256, 3584, 8192
QKV = QW + 2 * KW
FEW, MANY = 6, 20
TR, TC = 2048, 512
HT = 2
UT, UC = 7, 28
ONE, FIXES = 1, (3, 4, 5)
FIX = FIXES[-1]
ALL = ONE + FIX
SRC = 6
REST = NX - ALL
BUCKETS = (0, 1, 2, 4, 10)
SCALE = HD ** -0.5
EXP2 = SCALE * 1.4426950408889634
VM = pl.BlockSpec(memory_space=pltpu.VMEM)
HB = pl.BlockSpec(memory_space=pl.ANY)
SM = pl.BlockSpec(memory_space=pltpu.SMEM)
ROW = (ROWS, HD)
T_ORDER, T_START, T_COUNT, T_LIST, T_CODE, T_IDX, T_MISC, T_PAR = range(8)
DMA = pltpu.SemaphoreType.DMA


def coords():
    beam = lax.axis_index('beam')
    return beam // 2, lax.axis_index('sp'), beam % 2


def peer(x, y, c):
    return {'sp': y, 'beam': 2 * x + c}


def group_peers(x, y, c):
    return [(y, 1 - c), (1 - y, c), (1 - y, 1 - c)]


def all_peers(x, y, c):
    far = [(1 - x, yy, cc) for yy in (y, 1 - y) for cc in (c, 1 - c)]
    return far + [(x, yy, cc) for yy, cc in group_peers(x, y, c)]


def barrier_with(ids):
    sem = pltpu.get_barrier_semaphore()
    for dev in ids:
        pl.semaphore_signal(sem, inc=1, device_id=dev, device_id_type=MESH)
    pl.semaphore_wait(sem, len(ids))


def remote(src, dst, send_sem, recv_sem, dev):
    return pltpu.make_async_remote_copy(src_ref=src, dst_ref=dst, send_sem=send_sem, recv_sem=recv_sem,
                                        device_id=dev, device_id_type=MESH)


def ends(sem, *at):
    return sem.at[(0,) + at], sem.at[(1,) + at]


def local(src, dst, sem):
    return pltpu.make_async_copy(src, dst, sem)


def span(i, size):
    return pl.ds(pl.multiple_of(i * size, size), size)


def cols(i, size):
    return slice(i * size, (i + 1) * size)


def rsum(v):
    return jnp.sum(v, axis=-1, keepdims=True)


def rmax(v):
    return jnp.max(v, axis=-1, keepdims=True)


def csum(v):
    return jnp.sum(v, axis=0, keepdims=True)


def iota(shape_, dim):
    return lax.broadcasted_iota(I32, shape_, dim)


def mm(a, b):
    return jnp.dot(a, b, preferred_element_type=F32)


def start_all(copies):
    for cp in copies:
        cp.start()
    return copies


def wait_all(copies):
    for cp in copies:
        cp.wait()


class Stream:
    def __init__(self, wbuf, wsem, phases, ref_like):
        self.wbuf, self.wsem, self.like, self.depth = wbuf, wsem, ref_like, wbuf.shape[0]
        self.phases, base = [], 0
        for count, issue in phases:
            self.phases.append((base, count, issue))
            base += count
        self.total = base

    def issue(self, t, slot, lo, hi):
        for base, count, fetch in self.phases:
            if base + count <= lo or hi < base:
                continue
            if lo == hi or (base <= lo and hi < base + count):
                fetch(t - base, self.wbuf.at[slot], self.wsem.at[slot])
            else:
                @pl.when((t >= base) & (t < base + count))
                def _(base=base, fetch=fetch):
                    fetch(t - base, self.wbuf.at[slot], self.wsem.at[slot])

    def prologue(self):
        for t in range(min(self.depth, self.total)):
            self.issue(t, t, t, t)

    def run(self, phase, group, body):
        base, count, _ = self.phases[phase]

        @pl.loop(0, count // group)
        def _(i):
            first = i * group + base
            slots = [(first + k) % self.depth for k in range(group)]
            for slot in slots:
                local(self.like, self.wbuf.at[slot], self.wsem.at[slot]).wait()
            body(i, [self.wbuf.at[slot] for slot in slots])
            for k, slot in enumerate(slots):
                self.issue(first + k + self.depth, slot, base + self.depth, base + count - 1 + self.depth)


def col_tiles(w_ref, layer, g, width, row_chunks):
    def issue(i, buf, sem):
        ci, ri = i // row_chunks, i % row_chunks
        at = pl.ds(pl.multiple_of(g * width + ci * TC, TC), TC)
        src = w_ref.at[span(ri, TR), at] if layer < 0 else w_ref.at[layer, span(ri, TR), at]
        local(src, buf, sem).start()
    return issue


def kv_tiles(wk_ref, wv_ref, layer, g):
    def issue(i, buf, sem):
        for k, w_ref in enumerate((wk_ref, wv_ref)):
            local(w_ref.at[layer, span(i, TR), span(g, KW)], buf.at[:, pl.ds(k * KW, KW)], sem).start()
    return issue


def gate_up_tiles(wg_ref, wu_ref, layer, g):
    def issue(i, buf, sem):
        at = pl.ds(pl.multiple_of(g * FW + (i // G) * TC, TC), TC)
        for k, w_ref in enumerate((wg_ref, wu_ref)):
            @pl.when((i // HT) % 2 == k)
            def _():
                local(w_ref.at[layer, span(i % HT, TR), at], buf, sem).start()
    return issue


def norm_into(r_ref, g_row, hbuf):
    total = rsum(r_ref[0] * r_ref[0])
    for k in range(1, G):
        total = total + rsum(r_ref[k] * r_ref[k])
    inv = lax.rsqrt(total / D + NORM_EPS)
    for k in range(G):
        gain = g_row(cols(k, QW)).astype(F32)
        hbuf[k // 2, :, cols(k % 2, QW)] = (r_ref[k] * inv * gain).astype(BF16)


def rope(x_bf, cos_row, sin_row):
    v = x_bf.astype(F32)
    return (v * cos_row + pltpu.roll(v, HALF, 1) * sin_row).astype(BF16)


def stream_q(stream, part, hbuf, acc, cos_row, sin_row, out_ref, first=0):
    def body(i, w):
        acc[i + HT * part] = mm(hbuf[0], w[0][:]) + mm(hbuf[1], w[1][:])

    stream.run(first + part, HT, body)
    for head in (range(KVH), range(KVH, QKV // HD))[part]:
        piece = acc[head // G, :, cols(head % G, HD)].astype(BF16)
        if head * HD < QW + KW:
            piece = rope(piece, cos_row, sin_row)
        out_ref[:, cols(head, HD)] = piece


def my_half(piece, c):
    wide = piece.astype(F32)
    return jnp.where(c == 0, wide[:NB], wide[NB:])


def spread_kv(buf, base, c, out_ref, at):
    for k in range(G):
        for j in range(G):
            part, h = j // 2, j % 2
            out_ref[:, at + part * KVH + 2 * k + h, :] = my_half(buf[base + k, :, QW + j * HD:QW + (j + 1) * HD], c)


def own_start(buf, g, sems, k0, peers, x):
    return start_all([remote(buf.at[g], buf.at[g], *ends(sems, k0, k), peer(x, *p))
                      for k, p in enumerate(peers)])


def kernel_table(par_ref, meta_ref, choice_ref, bucket_ref):
    square = (NA, NA)
    i, j = iota(square, 0), iota(square, 1)
    par_row = jnp.broadcast_to(par_ref[:], square)
    par_col = rsum(jnp.where(i == j, par_row, 0).astype(F32)).astype(I32)
    fi, fj = i.astype(F32), j.astype(F32)

    def flag(v):
        return jnp.where(v, 1.0, 0.0)

    same, same_t = par_col == j, par_row == i
    far, half = (i // NX) != (j // NX), (i // NX) == (j // NX)
    before = rsum(flag((par_row < par_col) | ((par_row == par_col) & (j < i))))
    cross_row = jnp.minimum(csum(flag(same & far)), 1.0)
    cross_col = jnp.minimum(rsum(flag(same_t & far)), 1.0)
    place_col = rsum(flag(half & (j < i)) * cross_row)
    slot_col = place_col + (i // NX * NX).astype(F32)[:, :1]
    code = jnp.where(par_row // NB == j // NB, 0.0, jnp.where(par_row // NX == j // NX, 1.0, 2.0))[:1]
    place_par = csum(flag(same_t) * place_col)
    lane = j[:1]
    used = [rsum(jnp.where(lane // NX == k, cross_row, 0.0)) for k in range(2)]
    extra = jnp.maximum(used[0], used[1]) - ALL
    most = extra + FIX
    bucket = flag(extra > BUCKETS[0])
    choice = flag(most > FIXES[0]) + flag(most > FIXES[1])
    choice_ref[0] = choice.astype(I32)[0, 0]
    for n in BUCKETS[1:]:
        bucket = bucket + flag(extra > n)
    bucket_ref[0] = bucket.astype(I32)[0, 0]
    misc = jnp.where(lane == 0, used[0], used[1])
    rows = [csum(jnp.where(before == fj, fi, 0.0)), csum(flag(par_col < j)), csum(flag(same)),
            csum(jnp.where(slot_col == fj, fi, 0.0) * cross_col), code,
            jnp.where(code > 1.0, place_par, (par_row % NB).astype(F32)[:1]), misc, par_row[:1].astype(F32)]
    for k, row in enumerate(rows):
        meta_ref[k:k + 1, :NA] = row.astype(I32)


def kernel_a(tok_ref, score_ref, cos_ref, sin_ref, ga_ref, wq_ref, wk_ref, wv_ref, k_ref, v_ref,
             q_out, kv_out, own_out, r_out, score_out, xp_out,
             wbuf, wsem, tokx, scx, r_s, hbuf, acc, qkvx, ssem, rsem, xsem):
    x, y, c = coords()
    g = y * 2 + c
    d = x * G + g
    stream = Stream(wbuf, wsem, [(G, col_tiles(wq_ref, 0, g, QW, HT)), (HT, kv_tiles(wk_ref, wv_ref, 0, g))],
                    wq_ref.at[0, pl.ds(0, TR), pl.ds(0, TC)])
    stream.prologue()
    others = all_peers(x, y, c)
    barrier_with([peer(*p) for p in others])
    tok_copy = remote(tok_ref, tokx, ssem.at[0], rsem.at[0], peer(x, y, 1 - c))
    tok_copy.start()
    beam = 2 * x + c
    for i in range(NB):
        scx[beam, i:i + 1, :] = jnp.full((1, HD), score_ref[i], F32)
    for k in range(G):
        r_s[k, span(c, NB), :] = tok_ref[:, cols(k, QW)].astype(F32)
    sc_copies = start_all([remote(scx.at[beam], scx.at[beam], ssem.at[k], rsem.at[k], peer(xx, y, cc))
                           for k, (xx, cc) in enumerate(((1 - x, c), (1 - x, 1 - c), (x, 1 - c)), 1)])
    beside = peer(x, y, 1 - c)
    for k, ref in enumerate((k_ref, v_ref)):
        @pl.when(1 - c == k)
        def _():
            @pl.loop(0, NB)
            def _(r):
                remote(ref.at[1, r], xp_out.at[r], xsem.at[0], xsem.at[1], beside).start()

    tok_copy.wait()
    for k in range(G):
        r_s[k, span(1 - c, NB), :] = tokx[:, cols(k, QW)].astype(F32)
    norm_into(r_s, lambda at: ga_ref[0:1, at], hbuf)
    for i in range(HT):
        stream_q(stream, i, hbuf, acc, cos_ref[:], sin_ref[:], qkvx.at[d])
        own = qkvx.at[d]
        piece = own.at[:, pl.ds(0, QW)] if i == 0 else own.at[:, pl.ds(QW, 2 * KW)]
        copies = start_all([remote(piece, piece, ssem.at[G * (i + 1) + k], rsem.at[G * (i + 1) + k], peer(*p))
                            for k, p in enumerate(others) if i == 0 or k >= G])
        if i == 0:
            q_copies = copies
    own_out[:] = qkvx[d]
    r_out[:] = r_s[:]
    wait_all(sc_copies)
    for k in range(G):
        score_out[cols(k, NB), :] = scx[k]

    def spread_q(dd):
        for h in range(KVH):
            q_out[span(dd // G, NX), dd % G * KVH + h, :] = qkvx[dd, :, cols(h, HD)].astype(F32)

    spread_q(d)
    wait_all(copies)
    spread_kv(qkvx, x * G, c, kv_out, 0)
    for k in range(len(others) - 1, -1, -1):
        q_copies[k].wait()
        xx, yy, cc = others[k]
        spread_q(xx * G + yy * 2 + cc)
    remote(xp_out, xp_out, xsem.at[0], xsem.at[1], beside).wait()


def mask_bias(limit):
    row, col = iota((NA, ROWS), 0), iota((NA, ROWS), 1)
    ok = ((col % KVH) == (row // G)) & (col < limit * KVH)
    return jnp.where(ok, 0.0, NEG)


def attend(q, k_rows, v_rows, bias):
    s = lax.dot_general(q, k_rows, (((1,), (1,)), ((), ())), preferred_element_type=F32)
    s = (s.reshape(-1, NA, ROWS) + bias[:]).reshape(s.shape)
    m = rmax(s)
    e = jnp.exp2((s - m) * EXP2)
    return mm(e.astype(BF16), v_rows), m * SCALE, rsum(e)


def to_lanes(column):
    return csum(jnp.where(iota((NA, HD), 0) == iota((NA, HD), 1), column, 0.0))


def keep(o_ref, st_ref, b, o, m, total):
    o_ref[b] = o
    st_ref[0, pl.ds(b, 1), :] = to_lanes(m)
    st_ref[1, pl.ds(b, 1), :] = to_lanes(total)


def kernel_home(meta, pos_ref, q_ref, k_ref, v_ref, xp_ref, o_ref, st_ref, fix, rest, kbuf, vbuf, bias, ksem, vsem, pbuf, pisem, posem):
    x, y, c = coords()
    pack = Pack(1, meta, k_ref, v_ref, xp_ref, ((fix, ONE, ALL), (rest, ALL, NX)), pbuf, pisem, posem, ONE, NX)
    first = (2 * x + c) * NB
    limit = jnp.clip(pos_ref[0] - y * SLOTS, 0, SLOTS)

    def count_of(r):
        return jnp.where(limit > 0, meta[T_COUNT, first + r], 0)

    def copies(r):
        return local(k_ref.at[0, r], kbuf.at[r], ksem.at[r]), local(v_ref.at[0, r], vbuf.at[r], vsem.at[r])

    @pl.loop(0, NB)
    def _(r):
        @pl.when(count_of(r) > 0)
        def _():
            start_all(copies(r))

    pack.fetch()
    o_ref[:] = jnp.zeros_like(o_ref)
    st_ref[0] = jnp.full((NA, HD), NEG, F32)
    st_ref[1] = jnp.zeros((NA, HD), F32)
    bias[:] = mask_bias(limit)

    @pl.loop(0, NB)
    def _(r):
        count = count_of(r)
        start = meta[T_START, first + r]

        @pl.when(count > 0)
        def _():
            wait_all(copies(r))

        def step(s, carry):
            beams = [meta[T_ORDER, start + jnp.minimum(s * G + j, count - 1)] for j in range(G)]
            q = jnp.concatenate([q_ref[b] for b in beams], axis=0).astype(BF16)
            o, m, total = attend(q, kbuf[r], vbuf[r], bias)
            for j, b in enumerate(beams):
                at = cols(j, NA)
                keep(o_ref, st_ref, b, o[at], m[at], total[at])
            return carry

        lax.fori_loop(0, (count + G - 1) // G, step, 0)

        @pl.when(r == G)
        def _():
            pack.move()

    pack.finish()


def lane_pick(rows, lane):
    return rsum(jnp.where(iota(rows.shape, 1) == lane, rows, 0.0))


def send_partials(o_ref, st_ref, ox, sx, om, sm, x, y, c, psem):
    g = y * 2 + c
    far = span(1 - x, NX)
    beside = peer(x, y, 1 - c)
    merge = [remote(st_ref.at[:, far, :], sm, *ends(psem, 0, 0), beside)]
    for yy in range(2):
        merge.append(remote(o_ref.at[far, span(yy * 2 + 1 - c, KVH), :], om.at[yy], *ends(psem, 1, yy), beside))
    start_all(merge)
    near, copies = span(x, NX), []
    for k, (yy, cc) in enumerate(group_peers(x, y, c), 2):
        dev = peer(x, yy, cc)
        copies.append(remote(st_ref.at[:, near, :], sx.at[g], *ends(psem, 0, k), dev))
        copies.append(remote(o_ref.at[near, span(yy * 2 + cc, KVH), :], ox.at[g], *ends(psem, 1, k), dev))
    start_all(copies)
    sx[g] = st_ref[:, near, :]
    ox[g] = o_ref[near, span(g, KVH), :]
    wait_all(merge)
    sm[0] = jnp.maximum(sm[0], st_ref[0, far, :])
    sm[1] = sm[1] + st_ref[1, far, :]
    for yy in range(2):
        om[yy] = om[yy] + o_ref[far, span(yy * 2 + c, KVH), :]
    across = []
    for k, dy in enumerate((0, 1), 5):
        yy = (y + dy) % 2
        dev = peer(1 - x, yy, c)
        across.append(remote(sm, sx.at[G + y], *ends(psem, 0, k), dev))
        across.append(remote(om.at[yy], ox.at[G + y], *ends(psem, 1, k), dev))
    return copies + start_all(across)


def combine_first(copies, own_ref, ox, sx, g, out_ref):
    lanes = iota((NX, HD), 1)
    s_self = jnp.full((NX, HD), NEG, F32)
    for h in range(KVH):
        q = own_ref[:, cols(h, HD)].astype(F32)
        kk = own_ref[:, cols(KVH + h // G, HD)].astype(F32)
        s_self = jnp.where(lanes == g * KVH + h, rsum(q * kk) * SCALE, s_self)
    wait_all(copies)
    top = s_self
    for i in range(SRC):
        top = jnp.maximum(top, sx[i, 0])
    e_self = jnp.exp(s_self - top)
    total = e_self
    weights = []
    for i in range(SRC):
        weights.append(jnp.exp(sx[i, 0] - top))
        total = total + weights[i] * sx[i, 1]
    for h in range(KVH):
        lane = g * KVH + h
        vv = own_ref[:, cols(KVH + 2 + h // G, HD)].astype(F32)
        mix = lane_pick(e_self, lane).astype(BF16).astype(F32) * vv
        for i in range(SRC):
            mix = mix + lane_pick(weights[i], lane) * ox[i, :, h, :]
        out_ref[:, cols(h, HD)] = (mix / lane_pick(total, lane)).astype(BF16)


class Crossing:
    def __init__(self, x, y, c, rows, sems):
        self.first, self.second = [], []
        for k, (src, got, passed) in enumerate(rows):
            if src is not got:
                self.first.append(remote(src, got, *ends(sems, k), peer(1 - x, y, c)))
            self.second.append(remote(got, passed, sems.at[2, k], sems.at[3, k], peer(x, y, 1 - c)))
        self.ready = len(self.second) - len(self.first)

    def start(self):
        start_all(self.first)
        start_all(self.second[:self.ready])

    def forward(self, k):
        self.first[k].wait_recv()
        self.second[self.ready + k].start()

    def finish(self, k):
        for i in range(k, len(self.first)):
            self.forward(i)
        for cp in self.first:
            cp.wait_send()
        wait_all(self.second)


def fix_rows(n, fix_ref, fix_r, fix_p):
    return [(fix_ref.at[k], fix_r.at[k], fix_p.at[k]) for k in range(n)]


def out_mlp(stream, first, g, x, peers, r_s, hbuf, acc, ox, yx, zx, ubuf, gm_row, sems, usem, cross, side):
    def half_sends(buf, k0, i):
        buf[g, i] = acc[i].astype(BF16)
        start_all([remote(buf.at[g, i], buf.at[g, i], *ends(sems, k0, k), peer(x, *p))
                   for k, p in enumerate(peers)])

    def add(buf, k0):
        wait_all([remote(buf.at[g], buf.at[g], *ends(sems, k0, k), peer(x, *p)) for k, p in enumerate(peers)])
        for k in range(G):
            for i in range(HT):
                r_s[k, :, cols(i, TC)] = r_s[k, :, cols(i, TC)] + buf[k, i].astype(F32)

    copies = own_start(ox, g, sems, 0, peers, x)
    wait_all(copies)
    for k in range(G):
        hbuf[k // 2, :, cols(k % 2, QW)] = ox[k]

    def project(w):
        return mm(hbuf[0], w[0][:]) + mm(hbuf[1], w[1][:])

    def body_out(i, w):
        acc[i] = project(w)
        half_sends(yx, 1, i)

    stream.run(first, HT, body_out)
    add(yx, 1)
    norm_into(r_s, gm_row, hbuf)

    def body_gu(i, w):
        side(6 + 2 * i, KVH + 2 * i)
        gate = project(w[:HT]).astype(BF16).astype(F32)
        up = project(w[HT:]).astype(BF16).astype(F32)
        at = g * UT + i
        ubuf[at] = (jax.nn.silu(gate) * up).astype(BF16)
        start_all([remote(ubuf.at[at], ubuf.at[at], *ends(usem, k), peer(x, *p))
                   for k, p in enumerate(peers)])

    stream.run(first + 1, G, body_gu)
    cross.forward(0)
    mine = ubuf.at[pl.ds(g * UT, UT)]
    wait_all([remote(mine, mine, *ends(usem, k), peer(x, *p)) for k, p in enumerate(peers)])

    def body_down(i, w):
        side(20 + G * i, G * 6)
        total = mm(ubuf[0], w[0][cols(0, TC), :])
        for k in range(1, UC):
            total = total + mm(ubuf[k], w[k // G][cols(k % G, TC), :])
        acc[i] = total
        half_sends(zx, 2, i)

    stream.run(first + 2, UT, body_down)
    add(zx, 2)


def mlp_phases(layer, g, wo_ref, wg_ref, wu_ref, wd_ref):
    return [(G, col_tiles(wo_ref, layer, g, QW, HT)),
            (UC, gate_up_tiles(wg_ref, wu_ref, layer, g)),
            (2 * UT, col_tiles(wd_ref, layer, g, QW, UT))]


def kernel_mid(n, o_ref, st_ref, own_ref, r_ref, cos_ref, sin_ref, ga_ref, gm_ref, wo_ref, wg_ref, wu_ref, wd_ref, wq_ref, wk_ref, wv_ref,
               k_ref, v_ref, one_ref, fix_ref,
               qkv_out, r_out, one_p, fix_r, fix_p, xq1_out, xp0_out, xq0_out,
               wbuf, wsem, r_s, hbuf, acc, ox, yx, zx, ubuf, qkvx, px, sx, om, sm, sems, usem, csem, xsem, psem):
    x, y, c = coords()
    g = y * 2 + c
    peers = group_peers(x, y, c)
    stream = Stream(wbuf, wsem, mlp_phases(0, g, wo_ref, wg_ref, wu_ref, wd_ref) + [
        (G, col_tiles(wq_ref, 1, g, QW, HT)), (HT, kv_tiles(wk_ref, wv_ref, 1, g))],
        wq_ref.at[0, pl.ds(0, TR), pl.ds(0, TC)])
    stream.prologue()
    beside = peer(x, y, 1 - c)
    others = all_peers(x, y, c)
    barrier_with([peer(*p) for p in others])
    here = one_ref.at[0]
    cross = Crossing(x, y, c, [(here, here, one_p.at[0])] + fix_rows(n, fix_ref, fix_r, fix_p), csem)
    partials = send_partials(o_ref, st_ref, px, sx, om, sm, x, y, c, psem)
    cross.start()
    r_s[:] = r_ref[:]

    others_rows = ((1, c, xq1_out), (0, 1 - c, xp0_out), (0, c, xq0_out))

    def side(lo, hi):
        @pl.loop(lo, hi)
        def _(q):
            for at, (layer, part, out) in enumerate(others_rows):
                for k, ref in enumerate((k_ref, v_ref)):
                    @pl.when((q // NB == at) & (part == k))
                    def _():
                        remote(ref.at[layer, q % NB], out.at[q % NB], *ends(xsem, at), beside).start()

    side(0, 6)
    combine_first(partials, own_ref, px, sx, g, ox.at[g])
    out_mlp(stream, 0, g, x, peers, r_s, hbuf, acc, ox, yx, zx, ubuf, lambda at: gm_ref[0:1, at], sems, usem, cross, side)
    cross.forward(1)
    norm_into(r_s, lambda at: ga_ref[1:2, at], hbuf)
    for i in range(HT):
        stream_q(stream, i, hbuf, acc, cos_ref[:], sin_ref[:], qkvx.at[g], 3)
        own = qkvx.at[g]
        piece = own.at[:, pl.ds(0, QW)] if i == 0 else own.at[:, pl.ds(QW, 2 * KW)]
        copies = start_all([remote(piece, piece, *ends(sems, 3 * i, k), peer(x, *p)) for k, p in enumerate(peers)])
        if i == 0:
            q_copies = copies
    cross.forward(2)
    r_out[:] = r_s[:]
    for k, (_, _, out) in enumerate(others_rows):
        remote(out, out, *ends(xsem, k), beside).wait()
    wait_all(q_copies + copies)
    for k in range(G):
        for h in range(KVH):
            qkv_out[:, k * KVH + h, :] = my_half(qkvx[k, :, cols(h, HD)], c)
    spread_kv(qkvx, 0, c, qkv_out, NA)
    cross.finish(3)


def kernel_end(n, o_ref, st_ref, r_ref, gm_ref, gf_ref, wo_ref, wg_ref, wu_ref, wd_ref, wvoc_ref,
               fix_ref,
               candx, log_out, fix_r, fix_p,
               wbuf, wsem, r_s, hbuf, acc, ox, yx, zx, ubuf, px, sx, lbuf, stx, run_st,
               sems, usem, psem, lsem, csem):
    x, y, c = coords()
    g = y * 2 + c
    peers = group_peers(x, y, c)
    stream = Stream(wbuf, wsem, mlp_phases(1, g, wo_ref, wg_ref, wu_ref, wd_ref) + [
        (VW // TC * HT, col_tiles(wvoc_ref, -1, g, VW, HT))],
        wvoc_ref.at[pl.ds(0, TR), pl.ds(0, TC)])
    stream.prologue()
    barrier_with([peer(x, *p) for p in peers] + [peer(1 - x, y, c)])
    cross = Crossing(x, y, c, fix_rows(n + ONE, fix_ref, fix_r, fix_p), csem)
    cross.start()
    copies = []
    for k, (yy, cc) in enumerate(peers):
        heads, dev = span(yy * 2 + cc, KVH), peer(x, yy, cc)
        copies.append(remote(st_ref, sx.at[g], *ends(psem, 0, k), dev))
        copies.append(remote(o_ref.at[:, heads, :], px.at[g], *ends(psem, 1, k), dev))
    start_all(copies)
    sx[g] = st_ref[:]
    px[g] = o_ref[:, span(g, KVH), :]
    r_s[:] = r_ref[:]
    wait_all(copies)
    for cc in range(2):
        pair = (cc, 2 + cc)
        top = jnp.maximum(sx[pair[0], 0], sx[pair[1], 0])
        weights = [jnp.exp(sx[p, 0] - top) for p in pair]
        total = weights[0] * sx[pair[0], 1] + weights[1] * sx[pair[1], 1]
        for h in range(KVH):
            lane = g * KVH + h
            mix = lane_pick(weights[0], lane) * px[pair[0], :, h, :] + lane_pick(weights[1], lane) * px[pair[1], :, h, :]
            acc[h // G, cols(cc, NB), cols(h % G, HD)] = mix / lane_pick(total, lane)
    for k in range(HT):
        ox[g, :, cols(k, TC)] = acc[k].astype(BF16)
    out_mlp(stream, 0, g, x, peers, r_s, hbuf, acc, ox, yx, zx, ubuf, lambda at: gm_ref[1:2, at], sems, usem, cross, lambda lo, hi: lo)
    cross.forward(1)
    norm_into(r_s, lambda at: gf_ref[at].reshape(1, QW), hbuf)
    run_st[0] = jnp.full((NX, HD), NEG, F32)
    run_st[1] = jnp.zeros((NX, HD), F32)
    nv = VW // TC

    def body_voc(i, w):
        logits = mm(hbuf[0], w[0][:]) + mm(hbuf[1], w[1][:])
        for cc in range(2):
            lbuf[i, cc] = logits[cols(cc, NB)]
        at = g * nv + i
        candx[at] = lbuf[i, c]
        start_all([remote(lbuf.at[i, cc], candx.at[at], *ends(lsem, k), peer(x, yy, cc))
                   for k, (yy, cc) in enumerate(peers)])
        @pl.when(i == nv // 2)
        def _():
            cross.forward(2)

        old = run_st[0][:, :1]
        top = jnp.maximum(old, rmax(logits))
        run_st[1] = run_st[1] * jnp.exp(old - top) + rsum(jnp.exp(logits - top))
        run_st[0] = jnp.broadcast_to(top, (NX, HD))

    stream.run(3, HT, body_voc)
    stx[g] = run_st[:]
    wait_all(own_start(stx, g, sems, 3, peers, x))
    tops = [stx[k, 0, span(c, NB), :] for k in range(G)]
    top = functools.reduce(jnp.maximum, tops)
    total = sum(stx[k, 1, span(c, NB), :] * jnp.exp(tops[k] - top) for k in range(G))
    log_out[:] = top + jnp.log(total)
    got = candx.at[pl.ds(g * nv, nv)]
    wait_all([remote(lbuf.at[:, cc], got, *ends(lsem, k), peer(x, yy, cc)) for k, (yy, cc) in enumerate(peers)])
    cross.finish(3)


class Pack:
    def __init__(self, layer, meta, k_ref, v_ref, xp_ref, segments, buf, isem, osem, lo, hi):
        self.lo, self.hi = lo, hi
        self.x, _, self.c = coords()
        self.layer, self.meta, self.own, self.xp = layer, meta, (k_ref, v_ref), xp_ref
        self.segments, self.buf, self.isem, self.osem = segments, buf, isem, osem

    def each(self, fn):
        lax.fori_loop(self.lo, jnp.minimum(self.meta[T_MISC, self.x], self.hi), lambda p, z: (fn(p), z)[1], 0)

    def fetch(self):
        self.each(self.fetch_one)

    def fetch_one(self, p):
        v = self.meta[T_LIST, self.x * NX + p]
        r, own = v % NB, (v // NB) % 2 == self.c
        for core, mine in enumerate(self.own):
            @pl.when((self.c == core) & own)
            def _():
                local(mine.at[self.layer, r], self.buf.at[p], self.isem.at[p]).start()

        @pl.when(jnp.logical_not(own))
        def _():
            local(self.xp.at[r], self.buf.at[p], self.isem.at[p]).start()

    def store(self, p, op):
        for ref, lo, hi in self.segments:
            @pl.when((p >= lo) & (p < hi))
            def _():
                op(local(self.buf.at[p], ref.at[jnp.clip(p - lo, 0, hi - lo - 1)], self.osem.at[p]))

    def move(self):
        def one(p):
            local(self.xp.at[0], self.buf.at[p], self.isem.at[p]).wait()
            self.store(p, lambda cp: cp.start())
        self.each(one)

    def finish(self):
        self.each(lambda p: self.store(p, lambda cp: cp.wait()))


def kernel_pack(meta, dep, k_ref, v_ref, xp_ref, one, buf, isem, osem):
    pack = Pack(1, meta, k_ref, v_ref, xp_ref, ((one, 0, ONE),), buf, isem, osem, 0, ONE)
    pack.fetch()
    pack.move()
    pack.finish()


def fetch_row(layer, meta, b, mine, own_ref, partner, crossed, dst, sem):
    code, idx = meta[T_CODE, b], meta[T_IDX, b]

    @pl.when(code == 0)
    def _():
        local(own_ref.at[layer, idx % NB], dst, sem).start()

    for ref, cond in zip(partner, (mine, jnp.logical_not(mine))):
        @pl.when((code == 1) & cond)
        def _():
            local(ref.at[idx % NB], dst, sem).start()

    for lo, hi, refs in crossed:
        for ref, cond in zip(refs, (mine, jnp.logical_not(mine))):
            @pl.when((code == 2) & (idx >= lo) & (idx < hi) & cond)
            def _():
                local(ref.at[jnp.clip(idx - lo, 0, hi - lo - 1)], dst, sem).start()


def put_new(buf, i, new, at):
    rows = span(at // 2, NX)
    hit = iota((NX, HD), 0) // KVH == at % 2
    both = jnp.concatenate([new, new], axis=0)
    buf[i, rows, :] = jnp.where(hit, both, buf[i, rows, :].astype(F32)).astype(BF16)


def kernel_child(layer, *refs):
    if layer:
        (meta, pos_ref, new_ref, score_ref, k_ref, v_ref, xp, xq, one_r, one_p, fix_r, fix_p, rest_r, rest_p, xp0,
         ko, vo, o_ref, st_ref, score_out, fix0, rest0, kbuf, vbuf, isem, osem, bias, pbuf, pisem, posem) = refs
        crossed = ((0, ONE, (one_r, one_p)), (ONE, ALL, (fix_r, fix_p)), (ALL, NX, (rest_r, rest_p)))
        pack = Pack(0, meta, k_ref, v_ref, xp0, ((fix0, 0, ALL), (rest0, ALL, NX)), pbuf, pisem, posem, 0, NX)
        at0 = NA
    else:
        (meta, pos_ref, new_ref, score_ref, logits_ref, log_ref, k_ref, v_ref, xp, xq, fix_r, fix_p, rest_r, rest_p, _, _,
         ko, vo, cand_ref, kbuf, vbuf, isem, osem, cand_buf, csem) = refs
        at0 = 0
        crossed = ((0, ALL, (fix_r, fix_p)), (ALL, NX, (rest_r, rest_p)))
    x, y, c = coords()
    first = (2 * x + c) * NB
    pos = pos_ref[0] - y * SLOTS
    both = ((k_ref, kbuf, ko), (v_ref, vbuf, vo))

    @pl.loop(0, NB)
    def _(i):
        for part, (src, buf, _) in enumerate(both):
            fetch_row(layer, meta, first + i, c == part, src, (xp, xq), crossed, buf.at[i], isem.at[part, i])

    if layer:
        pack.fetch()
        bias[:] = mask_bias(jnp.clip(pos + 1, 1, SLOTS))

    @pl.loop(0, NB)
    def _(i):
        for part, (src, buf, out) in enumerate(both):
            local(src.at[0, 0], buf.at[i], isem.at[part, i]).wait()

            @pl.when((pos >= 0) & (pos < SLOTS))
            def _():
                start = at0 + part * KVH
                put_new(buf, i, new_ref[i, start:start + KVH, :], jnp.clip(pos, 0, SLOTS - 1))

            local(buf.at[i], out.at[layer, i], osem.at[part, i]).start()
        if not layer:
            for k in range(KVH):
                at = i * KVH + k
                cand_buf[:, span(at, TC)] = score_ref[:, :1] + (logits_ref[at] - log_ref[:, :1])
            local(cand_buf.at[:, span(i, D)], cand_ref.at[:, span(i, D)], csem.at[0]).start()
        if layer:
            keep(o_ref, st_ref, i, *attend(new_ref[i, :NA, :].astype(BF16), kbuf[i], vbuf[i], bias))
            score_out[pl.ds(i, 1), :] = score_ref[pl.ds(meta[T_PAR, first + i], 1), :]

    if layer:
        pack.move()

    @pl.loop(0, NB)
    def _(i):
        for part, (_, buf, out) in enumerate(both):
            local(buf.at[i], out.at[layer, i], osem.at[part, i]).wait()

    if layer:
        pack.finish()
    else:
        local(cand_buf, cand_ref, csem.at[0]).wait()


def kernel_rest(n, src, got, passed, sems):
    x, y, c = coords()
    barrier_with([peer(1 - x, y, c), peer(x, y, 1 - c)])
    cross = Crossing(x, y, c, [(src.at[i], got.at[i], passed.at[i]) for i in range(n)], sems)
    cross.start()
    cross.finish(0)


def shape(s, t=BF16):
    return jax.ShapeDtypeStruct(s, t)


def rows_of(n):
    return shape((n,) + ROW)


def scratch_stream(n=MANY):
    return [pltpu.VMEM((n, TR, TC), BF16), DMA((n,))]


def scratch_mlp():
    wide = (G, NX, QW)
    return [pltpu.VMEM(wide, F32), pltpu.VMEM((HT, NX, TR), BF16), pltpu.VMEM((HT + 1, NX, TC), F32),
            pltpu.VMEM(wide, BF16), pltpu.VMEM((G, HT, NX, TC), BF16), pltpu.VMEM((G, HT, NX, TC), BF16),
            pltpu.VMEM((UC, NX, TC), BF16)]


def call(kernel, name, us, outs, ins, scratch, cid=-1, aliases=()):
    more = {} if cid < 0 else dict(collective_id=cid, has_side_effects=True)
    return pl.pallas_call(
        kernel, out_shape=tuple(o for o, _ in outs), in_specs=ins, out_specs=tuple(s for _, s in outs),
        scratch_shapes=scratch, input_output_aliases=dict(aliases), name=name,
        cost_estimate=pl.CostEstimate(flops=us * 400000000, bytes_accessed=us * 3000000, transcendentals=0),
        compiler_params=pltpu.CompilerParams(vmem_limit_bytes=123 * 2 ** 19, **more))


def solution(mesh):
    beam_spec = P(('dp', 'beam'))
    row_spec = P(('dp', 'beam'), None)
    cache_spec = P(None, ('dp', 'beam'), 'sp', None, None)
    full_rep = P()
    swap_x = [(b, (b + 2) % G) for b in range(G)]

    def rest(index, packed):
        def branch(k, n):
            outs = [(rows_of(REST), HB)] * 2
            if n == 0:
                return call(lambda *_: None, 'rest_none', 1, outs, [HB], [])
            return call(functools.partial(kernel_rest, n), f'rest_{n}', 1, outs, [HB], [DMA((4, n))], NX + k)
        return lax.switch(index, [branch(k, n) for k, n in enumerate(BUCKETS)], packed)

    def local_step(tok_emb, parent, position, beam_score, k_cache, v_cache, w_query, w_key, w_value, w_out, w_gate, w_up, w_down, g_attn, g_mlp, g_final, w_vocab):
        cur_pos = position[0]
        half = jnp.arange(HD, dtype=I32) % HALF
        inv_freq = ROPE_BASE ** (-2.0 * half.astype(F32) / HD)
        angles = (cur_pos.astype(F32) * inv_freq)[None, :]
        cos_row = jnp.cos(angles)
        sin_row = jnp.sin(angles) * jnp.where(jnp.arange(HD) < HALF, -1.0, 1.0)
        kc, vc = k_cache.reshape((2, NB) + ROW), v_cache.reshape((2, NB) + ROW)
        lanes = shape((NA, HD), F32)
        logits = shape((G * VW // TC, NB, TC), F32)

        meta, choice, bucket = call(kernel_table, 'table', 2, [(shape((NB, HD), I32), VM), (shape((1,), I32), SM), (shape((1,), I32), SM)], [VM], [])(parent)
        choice, bucket = choice.reshape(()), bucket.reshape(())

        def chosen(kernel, name, us, outs, ins, scratch, cid):
            return lambda *args: lax.switch(choice, [
                call(functools.partial(kernel, n), f'{name}_{n}', us, outs, ins, scratch, cid + n) for n in FIXES], *args)

        q0, kv0, own0, r0, scores, xp1 = call(
            kernel_a, 'qkv_first', 12,
            [(shape((NA, NA, HD), F32), VM), (shape((NB, NX, HD), F32), VM), (shape((NX, QKV)), VM),
             (shape((G, NX, QW), F32), VM), (lanes, VM), (rows_of(NB), HB)],
            [VM, SM, VM, VM, VM] + [HB] * 5,
            scratch_stream(FEW) + [
                pltpu.VMEM((NB, D), BF16), pltpu.VMEM((G, NB, HD), F32), pltpu.VMEM((G, NX, QW), F32),
                pltpu.VMEM((HT, NX, TR), BF16), pltpu.VMEM((HT + 1, NX, TC), F32), pltpu.VMEM((2 * G, NX, QKV), BF16),
                DMA((G * G,)), DMA((G * G,)), DMA((2,))], 1,
        )(tok_emb, beam_score, cos_row, sin_row, g_attn, w_query, w_key, w_value, kc, vc)

        pack_scratch = [pltpu.VMEM((NX,) + ROW, BF16), DMA((NX,)), DMA((NX,))]
        one1, = call(kernel_pack, 'pack_row', 3, [(rows_of(ONE), HB)],
                     [SM] + [HB] * 4, pack_scratch)(meta, own0, kc, vc, xp1)
        one_r1 = lax.ppermute(one1, 'beam', swap_x)
        o0, st0, fix1, rest1 = call(
            kernel_home, 'attend_home', 9,
            [(shape((NA, NA, HD), F32), VM), (shape((2, NA, HD), F32), VM), (rows_of(FIX), HB), (rows_of(REST), HB)],
            [SM, SM, VM, HB, HB, HB],
            [pltpu.VMEM((NB,) + ROW, BF16)] * 2 + [pltpu.VMEM((NA, ROWS), F32), DMA((NB,)), DMA((NB,))] + pack_scratch,
        )(meta, position, q0, kc, vc, xp1)


        weights = (w_out, w_gate, w_up, w_down)
        qkv1, r1, one_p1, fix_r1, fix_p1, xq1, xp0, xq0 = chosen(
            kernel_mid, 'mlp_first', 50,
            [(shape((NB, NA + NX, HD), F32), VM), (shape((G, NX, QW), F32), VM), (rows_of(ONE), HB),
             (rows_of(FIX), HB), (rows_of(FIX), HB)] + [(rows_of(NB), HB)] * 3,
            [VM] * 8 + [HB] * 11,
            scratch_stream() + scratch_mlp() + [
                pltpu.VMEM((G, NX, QKV), BF16), pltpu.VMEM((SRC, NX, KVH, HD), F32), pltpu.VMEM((SRC, 2, NX, HD), F32),
                pltpu.VMEM((2, NX, KVH, HD), F32), pltpu.VMEM((2, NX, HD), F32), DMA((2, G, 3)), DMA((2, 3)), DMA((4, ALL)), DMA((2, 3)), DMA((2, 2, 7))], 0,
        )(o0, st0, own0, r0, cos_row, sin_row, g_attn, g_mlp, *weights, w_query, w_key, w_value, kc, vc, one_r1, fix1)

        rest1, _ = lax.optimization_barrier((rest1, r1))
        rest_r1, rest_p1 = rest(bucket, rest1)

        child_scratch = [pltpu.VMEM((NB,) + ROW, BF16), pltpu.VMEM((NB,) + ROW, BF16), DMA((2, NB)), DMA((2, NB))]
        cache_out = [(shape((2, NB) + ROW), HB)] * 2
        ko, vo, o1, st1, score1, fix0, rest0 = call(
            functools.partial(kernel_child, 1), 'attend_child', 9,
            cache_out + [(shape((NB, NA, HD), F32), VM), (shape((2, NB, HD), F32), VM), (shape((NB, HD), F32), VM),
                         (rows_of(ALL), HB), (rows_of(REST), HB)],
            [SM, SM, VM, VM] + [HB] * 11, child_scratch + [pltpu.VMEM((NA, ROWS), F32)] + pack_scratch,
        )(meta, position, qkv1, scores, kc, vc, xp1, xq1, one_r1, one_p1, fix_r1, fix_p1, rest_r1, rest_p1, xp0)

        logit, log_z, fix_r0, fix_p0 = chosen(
            kernel_end, 'mlp_vocab', 58,
            [(logits, VM), (shape((NB, HD), F32), VM), (rows_of(ALL), HB), (rows_of(ALL), HB)],
            [VM] * 5 + [HB] * 6,
            scratch_stream() + scratch_mlp() + [
                pltpu.VMEM((G, NB, KVH, HD), F32), pltpu.VMEM((G, 2, NB, HD), F32),
                pltpu.VMEM((VW // TC, 2, NB, TC), F32), pltpu.VMEM((G, 2, NX, HD), F32),
                pltpu.VMEM((2, NX, HD), F32),
                DMA((2, G, 3)), DMA((2, 3)), DMA((2, 2, 3)), DMA((2, 3)), DMA((4, ALL))], 3,
        )(o1, st1, r1, g_mlp, g_final, *weights, w_vocab, fix0)

        rest0, log_z = lax.optimization_barrier((rest0, log_z))
        rest_r0, rest_p0 = rest(bucket, rest0)
        ko, vo, cand = call(
            functools.partial(kernel_child, 0), 'assemble_first', 8, cache_out + [(shape((NB, G * VW), F32), HB)],
            [SM, SM] + [VM] * 4 + [HB] * 10, child_scratch + [pltpu.VMEM((NB, G * VW), F32), DMA((1,))], -1, ((14, 0), (15, 1)),
        )(meta, position, kv0, score1, logit, log_z, kc, vc, xp0, xq0, fix_r0, fix_p0, rest_r0, rest_p0, ko, vo)
        return ko.reshape(k_cache.shape), vo.reshape(v_cache.shape), cand

    in_specs = (row_spec, P('dp', None), full_rep, beam_spec, cache_spec, cache_spec) + (full_rep,) * 11
    return jax.shard_map(local_step, mesh=mesh, in_specs=in_specs, out_specs=(cache_spec, cache_spec, row_spec), check_vma=False)
```
